32 devices in a mesh: site: 8 (over z, x), dom: 4 (over y, core).
Axes of the slice: x: 2, y: 2, z: 4, core: 2. Of those that a mesh axis runs over, the one named last changes fastest.
Arguments:
- top_partial: float32 [16, 61, 4, 8192], P(None, None, 'dom', 'site'), may hold values from 0.001 to 1
- bottom_partial: float32 [16, 61, 4, 8192], P(None, None, 'dom', 'site'), may hold values from 0.001 to 1
- left_vectors: float32 [256, 61, 61], P('dom'), may hold values from 0.05 to 1
- right_vectors: float32 [256, 61, 61], P('dom'), may hold values from 0.05 to 1
- decay_rates: float32 [256, 61], P('dom'), may hold values from 0.05 to 8
- state_weights: float32 [256, 61], P('dom'), may hold values from 0.002 to 0.05
- part_rates: float32 [256], P('dom'), may hold values from 0.3 to 3
- branch_lengths: float32 [1997], replicated, may hold values from 0.02 to 0.5
- pattern_weights: int32 [4, 8192], P('dom', 'site'), may hold values from 0 to 9
- block_partition: int32 [4, 64], P('dom', 'site'), may hold values from 0 to 255
- chosen_branches: int32 [16], replicated, may hold values from 0 to 1996, as said below
Outputs:
- site_loglik: float32 [16, 4, 8192], P(None, 'dom', 'site')
- part_derivs: float32 [2, 16, 256], P(None, None, 'dom')
- new_lengths: float32 [1997], replicated
The draws below stay inside these ranges and needn't reach their ends.
Inputs may be any that keep to these rules, and one draw needn't show every extreme that they name: `chosen_branches`: distinct branch numbers.
All inputs are finite; a program needn't handle non-finite values.
Results may differ from the reference program's by a relative error of at most 0.0003.
Values sent between devices are 32-bit elements; how exact they have to be, the bound alone decides.
No kernel may reach another device: no remote copies, remote signals or barrier semaphores. Data moves between devices by JAX's collectives and lax.ppermute only.
A program may use at most 64 MiB of HBM per device.

```python
import math
import jax
import jax.numpy as jnp
import numpy as np
from jax import lax

STATES = 61
BR = 16
BLK = 128
TREE_BR = 1997
PARTS_SIZE = 256
SG = 8192
NBLK_G = 64
N_DOM = 4


def draw_chosen_branches(key, part):
    picked = jax.random.permutation(jax.random.fold_in(key, 17), TREE_BR)
    return picked[:BR].astype(jnp.int32)


def with_ends(result, key, low, top_value):
    spot = [jax.random.randint(jax.random.fold_in(key, axis), (), 0, length) for axis, length in enumerate(result.shape)]
    longest = result.shape.index(max(result.shape))
    next_to = spot[:longest] + [(spot[longest] + 1) % result.shape[longest]] + spot[longest + 1:]
    return result.at[tuple(spot)].set(low).at[tuple(next_to)].set(top_value)


def block_levels(own_key, dims, shards, least, high):
    def one(position, parts):
        draws = jax.random.uniform(jax.random.fold_in(jax.random.fold_in(own_key, 6), position), (parts,), jnp.float32, least / len(shards), high / len(shards))
        return jnp.repeat(jnp.exp(draws), dims[position] // parts).reshape((-1,) + (1,) * (len(dims) - position - 1))

    level = one(*shards[0])
    for cut in shards[1:]:
        level = level * one(*cut)
    return level


def cumulative_ranks(count, skew):
    loads = [(1 << 20) // math.isqrt(standing ** skew) + 1 for standing in range(1, count + 1)]
    scale = 1 + sum(loads) // (1 << 30)
    return np.cumsum(np.array([max(1, weight // scale) for weight in loads]))


def ranked(key, extent, amount, slope):
    grid = cumulative_ranks(amount, slope)
    ticket = jax.random.randint(jax.random.fold_in(key, 1), extent, 0, int(grid[amount - 1]))
    standing = jnp.searchsorted(jnp.asarray(grid, jnp.int32), ticket, side="right")
    return jax.random.permutation(jax.random.fold_in(key, 2), amount)[standing].astype(jnp.int32)


def setup_inputs(seed: int = 0) -> dict:
    splits = jax.random.split(jax.random.key(seed), 12)
    top_partial = jnp.clip(jnp.exp(math.log(1.0) - 6.9077552 * jax.random.uniform(splits[0], (BR, STATES, N_DOM, SG), jnp.float32) ** block_levels(splits[0], (BR, STATES, N_DOM, SG), ((2, 4), (3, 8)), -0.2, 0.2)), 0.001, 1.0)
    bottom_partial = jnp.clip(jnp.exp(math.log(1.0) - 6.9077552 * jax.random.uniform(splits[1], (BR, STATES, N_DOM, SG), jnp.float32) ** block_levels(splits[1], (BR, STATES, N_DOM, SG), ((2, 4), (3, 8)), -0.2, 0.2)), 0.001, 1.0)
    left_vectors = jnp.clip(0.05 + 0.95 * jax.random.uniform(splits[2], (PARTS_SIZE, STATES, STATES), jnp.float32) ** block_levels(splits[2], (PARTS_SIZE, STATES, STATES), ((0, 4),), -0.2, 0.2), 0.05, 1.0)
    right_vectors = jnp.clip(0.05 + 0.95 * jax.random.uniform(splits[3], (PARTS_SIZE, STATES, STATES), jnp.float32) ** block_levels(splits[3], (PARTS_SIZE, STATES, STATES), ((0, 4),), -0.2, 0.2), 0.05, 1.0)
    decay_rates = jnp.clip(jnp.exp(math.log(8.0) - 5.075174 * jax.random.uniform(splits[4], (PARTS_SIZE, STATES), jnp.float32) ** block_levels(splits[4], (PARTS_SIZE, STATES), ((0, 4),), -0.2, 0.2)), 0.05, 8.0)
    state_weights = jnp.clip(jnp.exp(math.log(0.05) - 3.218876 * jax.random.uniform(splits[5], (PARTS_SIZE, STATES), jnp.float32) ** block_levels(splits[5], (PARTS_SIZE, STATES), ((0, 4),), -0.2, 0.2)), 0.002, 0.05)
    part_rates = jnp.clip(jnp.exp(math.log(3.0) - 2.3025851 * jax.random.uniform(splits[6], (PARTS_SIZE,), jnp.float32) ** block_levels(splits[6], (PARTS_SIZE,), ((0, 4),), -0.2, 0.2)), 0.3, 3.0)
    branch_lengths = jnp.clip(jnp.exp(jax.random.uniform(splits[7], (TREE_BR,), jnp.float32, math.log(0.02), math.log(0.5))), 0.02, 0.5)
    pattern_weights = with_ends(jax.random.randint(splits[8], (N_DOM, SG), 0, 10), jax.random.fold_in(splits[8], 1), 0, 9).astype(jnp.int32)
    block_partition = with_ends(ranked(splits[9], (N_DOM, NBLK_G), PARTS_SIZE, 2), jax.random.fold_in(splits[9], 3), 0, PARTS_SIZE - 1).astype(jnp.int32)
    chosen_branches = draw_chosen_branches(jax.random.fold_in(splits[11], 71), 0)
    return {"top_partial": top_partial, "bottom_partial": bottom_partial, "left_vectors": left_vectors, "right_vectors": right_vectors, "decay_rates": decay_rates, "state_weights": state_weights, "part_rates": part_rates, "branch_lengths": branch_lengths, "pattern_weights": pattern_weights, "block_partition": block_partition, "chosen_branches": chosen_branches}


def project(upper, lower, vec_left, vec_right, state_w):
    scaled = upper * jnp.transpose(state_w)[None, :, :, None]
    lefts = jnp.einsum('binl,nik->bknl', scaled, vec_left, precision=lax.Precision.HIGHEST)
    rights = jnp.einsum('nkj,bjnl->bknl', vec_right, lower, precision=lax.Precision.HIGHEST)
    return lefts, rights


def finish(lefts, rights, exponent, times, weight_f):
    joint = lefts * rights
    expo = jnp.transpose(exponent)[None, :, :, None]
    decayed = joint * jnp.exp(expo * times[:, None, None, None])
    like_zero = jnp.sum(decayed, axis=1)
    like_one = jnp.sum(decayed * expo, axis=1)
    like_two = jnp.sum(decayed * expo * expo, axis=1)
    first = like_one / like_zero
    second = like_two / like_zero - first * first
    loglik = weight_f[None] * jnp.log(like_zero)
    sums = jnp.stack([jnp.sum(weight_f[None] * first, axis=-1), jnp.sum(weight_f[None] * second, axis=-1)])
    return loglik, sums


def reference(top_partial, bottom_partial, left_vectors, right_vectors, decay_rates, state_weights, part_rates, branch_lengths, pattern_weights, block_partition, chosen_branches):
    times = branch_lengths[chosen_branches]
    upper_all = jnp.moveaxis(top_partial, 2, 0)
    lower_all = jnp.moveaxis(bottom_partial, 2, 0)

    def one_group(items):
        upper, lower, weights_g, blocks = items
        nblocks = blocks.shape[0]
        upper = upper.reshape(BR, STATES, nblocks, BLK)
        lower = lower.reshape(BR, STATES, nblocks, BLK)
        vec_left = left_vectors[blocks]
        vec_right = right_vectors[blocks]
        exponent = -decay_rates[blocks] * part_rates[blocks][:, None]
        lefts, rights = project(upper, lower, vec_left, vec_right, state_weights[blocks])
        weight_f = weights_g.astype(jnp.float32).reshape(nblocks, BLK)
        loglik, sums = finish(lefts, rights, exponent, times, weight_f)
        onehot = (blocks[:, None] == jnp.arange(PARTS_SIZE, dtype=jnp.int32)[None, :]).astype(jnp.float32)
        part_sums = jnp.einsum('abn,np->abp', sums, onehot, precision=lax.Precision.HIGHEST)
        return loglik.reshape(BR, nblocks * BLK), part_sums

    logliks, part_all = lax.map(one_group, (upper_all, lower_all, pattern_weights, block_partition))
    site_loglik = jnp.moveaxis(logliks, 0, 1)
    part_derivs = jnp.sum(part_all, axis=0)
    totals = jnp.sum(part_derivs, axis=2)
    updated = times - totals[0] / totals[1]
    new_lengths = branch_lengths.at[chosen_branches].set(updated)
    return site_loglik, part_derivs, new_lengths
```

```python
import functools

import jax
import jax.numpy as jnp
from jax import lax
from jax.experimental import pallas as pl
from jax.experimental.pallas import tpu as pltpu
from jax.sharding import PartitionSpec as P

BLK = 128
HALF = 64
F32 = jnp.float32
BF16 = jnp.bfloat16


def pack_kernel(rate_ref, left_ref, right_ref, decay_ref, weight_ref, out_ref):
    states, group, _ = left_ref.shape
    left = left_ref.reshape(states * group, states)
    right = right_ref.reshape(states * group, states)
    base = pl.program_id(0) * group
    for q in range(group):
        table = left[pl.ds(q, states, stride=group), :]
        decay = decay_ref[pl.ds(q, 1), :]
        rows = jnp.concatenate([table, decay, jnp.zeros((HALF - states - 1, states), F32)], axis=0)
        scale = jnp.concatenate(
            [
                weight_ref[pl.ds(q, 1), :],
                jnp.full((1, 1), -rate_ref[base + q], F32),
                jnp.zeros((1, HALF - states - 1), F32),
            ],
            axis=1,
        )
        scaled = rows.T * scale
        other = right[pl.ds(q, states, stride=group), :]
        tile = jnp.concatenate([scaled, other, jnp.zeros((states, HALF - states), F32)], axis=1)
        out_ref[q] = jnp.concatenate([tile, jnp.zeros((HALF - states, 2 * HALF), F32)], axis=0)


def pack_tables(left, right, decay, weight, rate):
    parts, states, _ = left.shape
    group = 8
    table = pl.BlockSpec((states, group, states), lambda g: (0, g, 0))
    row = pl.BlockSpec((group, states), lambda g: (g, 0))
    return pl.pallas_call(
        pack_kernel,
        grid=(parts // group,),
        in_specs=[pl.BlockSpec(memory_space=pltpu.SMEM), table, table, row, row],
        out_specs=pl.BlockSpec((group, HALF, 2 * HALF), lambda g: (g, 0, 0)),
        out_shape=jax.ShapeDtypeStruct((parts, HALF, 2 * HALF), F32),
        name="pack",
    )(rate, jnp.transpose(left, (1, 0, 2)), jnp.transpose(right, (1, 0, 2)), decay, weight)


def split_kernel(top_ref, bottom_ref, out_ref):
    nblocks = out_ref.shape[0]
    fused = out_ref.shape[2] // BLK
    states = top_ref.shape[0] // (nblocks * fused)
    pad = jnp.zeros((HALF - states, BLK), F32)
    for b in range(fused):
        for n in range(nblocks):
            for side, ref in enumerate((top_ref, bottom_ref)):
                rows = ref[pl.ds(b * states * nblocks + n, states, stride=nblocks), :]
                full = jnp.concatenate([rows, pad], axis=0)
                high = full.astype(BF16)
                low = (full - high.astype(F32)).astype(BF16)
                lanes = pl.ds(b * BLK, BLK)
                out_ref[n, pl.ds(side * HALF, HALF), lanes] = high
                out_ref[n, pl.ds((2 + side) * HALF, HALF), lanes] = low


def split_partials(top, bottom, branches, states, nblocks):
    fused = 2
    source = pl.BlockSpec((fused * states * nblocks, BLK), lambda b: (b, 0))
    return pl.pallas_call(
        split_kernel,
        grid=(branches // fused,),
        in_specs=[source, source],
        out_specs=pl.BlockSpec((nblocks, 4 * HALF, fused * BLK), lambda b: (0, 0, b)),
        out_shape=jax.ShapeDtypeStruct((nblocks, 4 * HALF, branches * BLK), BF16),
        name="split",
    )(top, bottom)


def pick_kernel(wanted_ref, where_ref, own_ref, partner_ref, out_ref, sems):
    owned = own_ref.shape[0]
    group = where_ref[0]
    me = where_ref[1]
    count = out_ref.shape[0]
    for n in range(count):
        part = wanted_ref[n]
        owner = part // owned
        row = part - owner * owned
        mine = owner == group + me

        @pl.when(mine)
        def _():
            pltpu.make_async_copy(own_ref.at[row], out_ref.at[n], sems.at[n]).start()

        @pl.when(jnp.logical_not(mine))
        def _():
            pltpu.make_async_copy(partner_ref.at[row], out_ref.at[n], sems.at[n]).start()

    for n in range(count):
        pltpu.make_async_copy(own_ref.at[0], out_ref.at[n], sems.at[n]).wait()


def pick_tiles(wanted, where, own, partner):
    count = wanted.shape[0]
    smem = pl.BlockSpec(memory_space=pltpu.SMEM)
    hbm = pl.BlockSpec(memory_space=pl.ANY)
    return pl.pallas_call(
        pick_kernel,
        in_specs=[smem, smem, hbm, hbm],
        out_specs=pl.BlockSpec(memory_space=pltpu.VMEM),
        out_shape=jax.ShapeDtypeStruct((count,) + own.shape[1:], F32),
        scratch_shapes=[pltpu.SemaphoreType.DMA((count,))],
        name="pick",
    )(wanted, where, own, partner)


def block_kernel(
    rounds, owned, pair, times_ref, blocks_ref, where_ref, weight_ref, operand_ref, *refs
):
    tiles = refs[: rounds]
    loglik_ref, share_ref = refs[rounds : rounds + 2]
    like_refs = refs[rounds + 2 :]
    states_lane = tiles[0].shape[2]
    n = pl.program_id(0)
    last = pl.num_programs(0) - 1
    branches = loglik_ref.shape[0]
    nblocks = loglik_ref.shape[1]
    distance = lax.rem(blocks_ref[n] // (owned * pair) - where_ref[2] + rounds, rounds)
    tile = tiles[0][0]
    for r in range(1, rounds):
        tile = jnp.where(distance == r, tiles[r][0], tile)
    lane = lax.broadcasted_iota(jnp.int32, tile.shape, 1)
    high = tile.astype(BF16)
    low = (tile - high.astype(F32)).astype(BF16)
    zero = jnp.zeros_like(high)
    is_left = lane < HALF
    left_high = jnp.where(is_left, high, zero)
    right_high = jnp.where(is_left, zero, high)
    left_low = jnp.where(is_left, low, zero)
    right_low = jnp.where(is_left, zero, low)
    first_rows = jnp.concatenate([left_high, right_high], axis=0)
    second_rows = jnp.concatenate([left_low, right_low], axis=0)
    lhs = jnp.concatenate(
        [
            jnp.concatenate([first_rows, first_rows], axis=1),
            jnp.concatenate([second_rows, jnp.zeros_like(second_rows)], axis=1),
        ],
        axis=0,
    )
    where_exponent = where_ref[3]
    column = jnp.sum(jnp.where(lane == where_exponent, tile, 0.0), axis=1, keepdims=True)
    expo = jnp.broadcast_to(column, (HALF, BLK))
    wide = 2 * BLK
    for c in range(branches * BLK // wide):
        prod = jnp.dot(
            lhs, operand_ref[0, :, c * wide : (c + 1) * wide], preferred_element_type=F32
        )
        lefts = prod[:HALF] + prod[2 * HALF : 3 * HALF]
        rights = prod[HALF : 2 * HALF] + prod[3 * HALF :]
        joint = lefts * rights
        for h in range(wide // BLK):
            b = c * (wide // BLK) + h
            zeroth = joint[:, h * BLK : (h + 1) * BLK] * jnp.exp(expo * times_ref[b])
            first = zeroth * expo
            second = first * expo
            for ref, term in zip(like_refs, (zeroth, first, second)):
                ref[b, pl.ds(n, 1), :] = jnp.sum(term, axis=0, keepdims=True)

    @pl.when(n == last)
    def _():
        weight = weight_ref[...].astype(F32)
        lanes = lax.broadcasted_iota(jnp.int32, (nblocks, BLK), 1)
        rows = lax.broadcasted_iota(jnp.int32, (nblocks, BLK), 0)
        ident = jnp.zeros((nblocks, BLK), F32)
        for m in range(nblocks):
            ident = jnp.where(rows == m, blocks_ref[m].astype(F32), ident)
        share = jnp.where(lanes == 2 * branches, ident, 0.0)
        for b in range(branches):
            like = like_refs[0][b]
            first = like_refs[1][b] / like
            second = like_refs[2][b] / like - first * first
            loglik_ref[b] = weight * jnp.log(like)
            one = jnp.sum(weight * first, axis=1, keepdims=True)
            two = jnp.sum(weight * second, axis=1, keepdims=True)
            share = jnp.where(lanes == b, one, share)
            share = jnp.where(lanes == branches + b, two, share)
        for d in range(share_ref.shape[0]):
            share_ref[d] = share


def block_likelihoods(times, blocks, where, weight, operand, tiles, owned, pair, devices):
    nblocks, depth, columns = operand.shape
    branches = times.shape[0]
    smem = pl.BlockSpec(memory_space=pltpu.SMEM)
    tile = pl.BlockSpec((1, HALF, 2 * HALF), lambda n: (n, 0, 0))
    whole = lambda shape: pl.BlockSpec(shape, lambda n: (0,) * len(shape))
    return pl.pallas_call(
        functools.partial(block_kernel, len(tiles), owned, pair),
        grid=(nblocks,),
        in_specs=[
            smem,
            smem,
            smem,
            whole((nblocks, BLK)),
            pl.BlockSpec((1, depth, columns), lambda n: (n, 0, 0)),
        ]
        + [tile] * len(tiles),
        out_specs=[whole((branches, nblocks, BLK)), whole((devices, nblocks, BLK))],
        out_shape=[
            jax.ShapeDtypeStruct((branches, nblocks, BLK), F32),
            jax.ShapeDtypeStruct((devices, nblocks, BLK), F32),
        ],
        scratch_shapes=[pltpu.VMEM((branches, nblocks, BLK), F32)] * 3,
        name="blocks",
    )(times, blocks, where, weight, operand, *tiles)


def sum_kernel(where_ref, share_ref, part_ref, total_ref):
    owned = part_ref.shape[1]
    terms = part_ref.shape[0]
    share = share_ref[...]
    rows = share.shape[0]
    lanes = lax.broadcasted_iota(jnp.int32, (rows, owned), 1) + where_ref[4]
    ident = share[:, terms : terms + 1].astype(jnp.int32)
    onehot = (ident == lanes).astype(F32)
    sums = lax.dot_general(
        share,
        onehot,
        (((0,), (0,)), ((), ())),
        precision=lax.Precision.HIGHEST,
        preferred_element_type=F32,
    )
    part_ref[...] = sums[:terms]
    total_ref[...] = jnp.sum(share, axis=0, keepdims=True)


def add_up(where, share, terms, owned):
    return pl.pallas_call(
        sum_kernel,
        in_specs=[
            pl.BlockSpec(memory_space=pltpu.SMEM),
            pl.BlockSpec(memory_space=pltpu.VMEM),
        ],
        out_specs=[pl.BlockSpec(memory_space=pltpu.VMEM)] * 2,
        out_shape=[
            jax.ShapeDtypeStruct((terms, owned), F32),
            jax.ShapeDtypeStruct((1, BLK), F32),
        ],
        name="sums",
    )(where, share)


def on_device(
    top_partial,
    bottom_partial,
    left_vectors,
    right_vectors,
    decay_rates,
    state_weights,
    part_rates,
    branch_lengths,
    pattern_weights,
    block_partition,
    chosen_branches,
):
    branches, states, _, sites_here = top_partial.shape
    nblocks = sites_here // BLK
    owned = left_vectors.shape[0]
    groups = lax.axis_size("dom")
    pair = 2 if groups % 2 == 0 else 1
    rounds = groups // pair
    me = lax.axis_index("dom")
    mine = me // pair
    where = jnp.stack(
        [mine * pair, me - mine * pair, mine, jnp.int32(states), me * owned]
    ).astype(jnp.int32)

    def shifted(value, r):
        step = [
            (d, ((d // pair + r) % rounds) * pair + d % pair) for d in range(groups)
        ]
        return lax.ppermute(value, "dom", step)

    blocks = block_partition[0]
    requests = [shifted(blocks, rounds - r) for r in range(1, rounds)]
    own = pack_tables(left_vectors, right_vectors, decay_rates, state_weights, part_rates)
    if pair == 2:
        partner = lax.ppermute(own, "dom", [(d, d ^ 1) for d in range(groups)])
    else:
        partner = own
    operand = split_partials(
        top_partial.reshape(branches * states * nblocks, BLK),
        bottom_partial.reshape(branches * states * nblocks, BLK),
        branches,
        states,
        nblocks,
    )
    answers = [
        shifted(pick_tiles(request, where, own, partner), r)
        for r, request in zip(range(1, rounds), requests)
    ]
    tiles = [pick_tiles(blocks, where, own, partner)]
    tiles += answers[::-1]
    times = branch_lengths[chosen_branches]
    devices = lax.axis_size("site") * groups
    loglik, share = block_likelihoods(
        times,
        blocks,
        where,
        pattern_weights.reshape(nblocks, BLK),
        operand,
        tiles,
        owned,
        pair,
        devices,
    )
    everything = lax.all_to_all(
        share, ("site", "dom"), split_axis=0, concat_axis=0, tiled=True
    )
    terms = 2 * branches
    parts, totals = add_up(
        where, everything.reshape(devices * nblocks, BLK), terms, owned
    )
    updated = times - totals[0, :branches] / totals[0, branches:terms]
    new_lengths = branch_lengths.at[chosen_branches].set(updated)
    return (
        loglik.reshape(branches, 1, sites_here),
        parts.reshape(2, branches, owned),
        new_lengths,
    )


def solution(mesh):
    return jax.shard_map(
        on_device,
        mesh=mesh,
        in_specs=(
            P(None, None, "dom", "site"),
            P(None, None, "dom", "site"),
            P("dom", None, None),
            P("dom", None, None),
            P("dom", None),
            P("dom", None),
            P("dom"),
            P(),
            P("dom", "site"),
            P("dom", "site"),
            P(),
        ),
        out_specs=(P(None, "dom", "site"), P(None, None, "dom"), P()),
        check_vma=False,
    )
```

```python
import functools

import jax
import jax.numpy as jnp
from jax import lax
from jax.experimental import pallas as pl
from jax.experimental.pallas import tpu as pltpu
from jax.sharding import PartitionSpec as P

BLK = 128
HALF = 64
F32 = jnp.float32
BF16 = jnp.bfloat16
LIMITS = pltpu.CompilerParams(vmem_limit_bytes=24 * 1024 * 1024)


def in_hbm(x):
    return pltpu.with_memory_space_constraint(x, pltpu.HBM)


def pack_kernel(
    rate_hbm,
    left_hbm,
    right_hbm,
    decay_hbm,
    weight_hbm,
    out_ref,
    rate_ref,
    left_ref,
    right_ref,
    decay_ref,
    weight_ref,
    small_sems,
    sems,
):
    states, parts, _ = left_ref.shape
    chunks = sems.shape[1]
    group = parts // chunks
    small = [
        pltpu.make_async_copy(src, dst, small_sems.at[i])
        for i, (src, dst) in enumerate(
            ((rate_hbm, rate_ref), (decay_hbm, decay_ref), (weight_hbm, weight_ref))
        )
    ]
    for copy in small:
        copy.start()

    def copies(g):
        rows = pl.ds(g * group, group)
        return [
            pltpu.make_async_copy(src.at[:, rows, :], dst.at[:, rows, :], sems.at[i, g])
            for i, (src, dst) in enumerate(((left_hbm, left_ref), (right_hbm, right_ref)))
        ]

    for g in range(chunks):
        for copy in copies(g):
            copy.start()
    for copy in small:
        copy.wait()
    left = left_ref.reshape(states * parts, states)
    right = right_ref.reshape(states * parts, states)
    for g in range(chunks):
        for copy in copies(g):
            copy.wait()
        for q in range(g * group, (g + 1) * group):
            table = left[pl.ds(q, states, stride=parts), :]
            decay = decay_ref[pl.ds(q, 1), :]
            rows = jnp.concatenate(
                [table, decay, jnp.zeros((HALF - states - 1, states), F32)], axis=0
            )
            scale = jnp.concatenate(
                [
                    weight_ref[pl.ds(q, 1), :],
                    jnp.full((1, 1), -rate_ref[q], F32),
                    jnp.zeros((1, HALF - states - 1), F32),
                ],
                axis=1,
            )
            scaled = rows.T * scale
            other = right[pl.ds(q, states, stride=parts), :]
            tile = jnp.concatenate(
                [scaled, other, jnp.zeros((states, HALF - states), F32)], axis=1
            )
            out_ref[q] = jnp.concatenate(
                [tile, jnp.zeros((HALF - states, 2 * HALF), F32)], axis=0
            )


def pack_tables(left, right, decay, weight, rate):
    parts, states, _ = left.shape
    chunks = parts // 8
    hbm = pl.BlockSpec(memory_space=pltpu.HBM)
    table = pltpu.VMEM((states, parts, states), F32)
    row = pltpu.VMEM((parts, states), F32)
    return pl.pallas_call(
        pack_kernel,
        in_specs=[hbm] * 5,
        out_specs=pl.BlockSpec(memory_space=pltpu.VMEM),
        out_shape=jax.ShapeDtypeStruct((parts, HALF, 2 * HALF), F32),
        scratch_shapes=[
            pltpu.SMEM((parts,), F32),
            table,
            table,
            row,
            row,
            pltpu.SemaphoreType.DMA((3,)),
            pltpu.SemaphoreType.DMA((2, chunks)),
        ],
        name="pack",
        compiler_params=LIMITS,
    )(
        in_hbm(rate),
        in_hbm(jnp.transpose(left, (1, 0, 2))),
        in_hbm(jnp.transpose(right, (1, 0, 2))),
        in_hbm(decay),
        in_hbm(weight),
    )


def start_tiles(wanted_ref, pair, own_ref, partner_ref, out_ref, sems):
    owned = own_ref.shape[0]
    me = lax.axis_index("dom")
    for n in range(out_ref.shape[0]):
        part = wanted_ref[n]
        owner = part // owned
        row = part - owner * owned
        mine = owner == me

        @pl.when(mine)
        def _():
            pltpu.make_async_copy(own_ref.at[row], out_ref.at[n], sems.at[n]).start()

        @pl.when(jnp.logical_not(mine))
        def _():
            pltpu.make_async_copy(partner_ref.at[row], out_ref.at[n], sems.at[n]).start()


def wait_tiles(own_ref, out_ref, sems):
    for n in range(out_ref.shape[0]):
        pltpu.make_async_copy(own_ref.at[0], out_ref.at[n], sems.at[n]).wait()


def pick_kernel(pair, wanted_ref, own_ref, partner_ref, out_ref, sems):
    start_tiles(wanted_ref, pair, own_ref, partner_ref, out_ref, sems)
    wait_tiles(own_ref, out_ref, sems)


def pick_tiles(wanted, own, partner, pair):
    count = wanted.shape[0]
    hbm = pl.BlockSpec(memory_space=pl.ANY)
    return pl.pallas_call(
        functools.partial(pick_kernel, pair),
        in_specs=[pl.BlockSpec(memory_space=pltpu.SMEM), hbm, hbm],
        out_specs=pl.BlockSpec(memory_space=pltpu.VMEM),
        out_shape=jax.ShapeDtypeStruct((count,) + own.shape[1:], F32),
        scratch_shapes=[pltpu.SemaphoreType.DMA((count,))],
        name="pick",
        compiler_params=LIMITS,
    )(wanted, own, partner)


def prepare_kernel(
    pair,
    rounds,
    blocks_ref,
    chosen_ref,
    lengths_ref,
    top_hbm,
    bottom_hbm,
    own_ref,
    partner_ref,
    out_ref,
    tiles_ref,
    aux_ref,
    map_ref,
    top_ref,
    bottom_ref,
    tile_sems,
    sems,
):
    nblocks = out_ref.shape[0]
    chunks = sems.shape[1]
    chunk = top_ref.shape[0] // chunks
    columns = out_ref.shape[3] // chunks
    fused = columns // BLK
    states = chunk // (fused * nblocks)
    branches = chosen_ref.shape[0]

    def copies(g):
        rows = pl.ds(g * chunk, chunk)
        return [
            pltpu.make_async_copy(src.at[rows], dst.at[rows], sems.at[i, g])
            for i, (src, dst) in enumerate(((top_hbm, top_ref), (bottom_hbm, bottom_ref)))
        ]

    for g in range(chunks):
        for copy in copies(g):
            copy.start()
    start_tiles(blocks_ref, pair, own_ref, partner_ref, tiles_ref, tile_sems)
    owned = own_ref.shape[0]
    my_pair = lax.axis_index("dom") // pair
    lane = lax.broadcasted_iota(jnp.int32, (1, BLK), 1)
    flat = lax.broadcasted_iota(jnp.int32, map_ref.shape, 0) * BLK
    flat = flat + lax.broadcasted_iota(jnp.int32, map_ref.shape, 1)
    for n in range(nblocks):
        part = blocks_ref[n]
        distance = lax.rem(part // (owned * pair) - my_pair + rounds, rounds)
        aux_ref[pl.ds(n, 1), :] = jnp.full((1, BLK), distance.astype(F32), F32)
        aux_ref[pl.ds(nblocks + n, 1), :] = jnp.full((1, BLK), part.astype(F32), F32)
    along = jnp.zeros((1, BLK), F32)
    update = jnp.zeros(map_ref.shape, jnp.int32)
    for b in range(branches):
        place = chosen_ref[b]
        time = lengths_ref[place]
        aux_ref[pl.ds(2 * nblocks + b, 1), :] = jnp.full((1, BLK), time, F32)
        along = jnp.where(lane == b, time, along)
        update = jnp.where(flat == place, b + 1, update)
    aux_ref[pl.ds(2 * nblocks + branches, 1), :] = along
    map_ref[...] = update
    pad = jnp.zeros((HALF - states, BLK), F32)

    def step(g, carry):
        for copy in copies(g):
            copy.wait()
        for b in range(fused):
            for n in range(nblocks):
                for side, ref in enumerate((top_ref, bottom_ref)):
                    first = g * chunk + b * states * nblocks + n
                    rows = ref[pl.ds(first, states, stride=nblocks), :]
                    full = jnp.concatenate([rows, pad], axis=0)
                    high = full.astype(BF16)
                    low = (full - high.astype(F32)).astype(BF16)
                    lanes = pl.ds(pl.multiple_of(g * columns + b * BLK, BLK), BLK)
                    out_ref[n, side, pl.ds(0, HALF), lanes] = high
                    out_ref[n, side, pl.ds(HALF, HALF), lanes] = low
        return carry

    lax.fori_loop(0, chunks, step, 0)
    wait_tiles(own_ref, tiles_ref, tile_sems)


def prepare(blocks, chosen, lengths, top, bottom, own, partner, states, pair, rounds):
    nblocks = blocks.shape[0]
    branches = chosen.shape[0]
    chunks = branches // 2
    smem = pl.BlockSpec(memory_space=pltpu.SMEM)
    hbm = pl.BlockSpec(memory_space=pltpu.HBM)
    anywhere = pl.BlockSpec(memory_space=pl.ANY)
    vmem = pl.BlockSpec(memory_space=pltpu.VMEM)
    rows = -(-lengths.shape[0] // BLK)
    return pl.pallas_call(
        functools.partial(prepare_kernel, pair, rounds),
        in_specs=[smem, smem, smem, hbm, hbm, anywhere, anywhere],
        out_specs=[vmem] * 4,
        out_shape=[
            jax.ShapeDtypeStruct((nblocks, 2, 2 * HALF, branches * BLK), BF16),
            jax.ShapeDtypeStruct((nblocks,) + own.shape[1:], F32),
            jax.ShapeDtypeStruct((2 * nblocks + branches + 8, BLK), F32),
            jax.ShapeDtypeStruct((rows, BLK), jnp.int32),
        ],
        scratch_shapes=[
            pltpu.VMEM(top.shape, F32),
            pltpu.VMEM(top.shape, F32),
            pltpu.SemaphoreType.DMA((nblocks,)),
            pltpu.SemaphoreType.DMA((2, chunks)),
        ],
        name="prepare",
        compiler_params=LIMITS,
    )(blocks, chosen, lengths, in_hbm(top), in_hbm(bottom), own, partner)


def block_kernel(rounds, states, aux_ref, weight_ref, operand_ref, *refs):
    tiles = refs[:rounds]
    loglik_ref, share_ref = refs[rounds : rounds + 2]
    like_refs = refs[rounds + 2 :]
    branches, nblocks, _ = loglik_ref.shape
    wide = 2 * BLK
    lane = lax.broadcasted_iota(jnp.int32, (HALF, 2 * HALF), 1)
    is_left = lane < HALF
    for n in range(nblocks):
        distance = aux_ref[pl.ds(n, 1), :]
        tile = tiles[0][n]
        for r in range(1, rounds):
            tile = jnp.where(distance == float(r), tiles[r][n], tile)
        turned = pltpu.roll(tile, HALF, 1)
        sides = []
        for double in (jnp.where(is_left, tile, turned), jnp.where(is_left, turned, tile)):
            high = double.astype(BF16)
            low = (double - high.astype(F32)).astype(BF16)
            sides.append(jnp.concatenate([high, low[:, :HALF]], axis=1))
        expo = jnp.broadcast_to(tile[:, states : states + 1], (HALF, BLK))
        for c in range(branches * BLK // wide):
            columns = pl.ds(c * wide, wide)
            prods = []
            for side, lhs in enumerate(sides):
                part = operand_ref[n, side, :, columns]
                rhs = jnp.concatenate([part, part[:HALF]], axis=0)
                prods.append(jnp.dot(lhs, rhs, preferred_element_type=F32))
            joint = prods[0] * prods[1]
            for h in range(wide // BLK):
                b = c * (wide // BLK) + h
                time = aux_ref[pl.ds(2 * nblocks + b, 1), :]
                zeroth = joint[:, h * BLK : (h + 1) * BLK] * jnp.exp(expo * time)
                first = zeroth * expo
                second = first * expo
                for ref, term in zip(like_refs, (zeroth, first, second)):
                    ref[b, pl.ds(n, 1), :] = jnp.sum(term, axis=0, keepdims=True)

    weight = weight_ref[...].astype(F32)
    lanes = lax.broadcasted_iota(jnp.int32, (nblocks, BLK), 1)
    share = jnp.where(lanes == 2 * branches, aux_ref[pl.ds(nblocks, nblocks), :], 0.0)
    for b in range(branches):
        like = like_refs[0][b]
        first = like_refs[1][b] / like
        second = like_refs[2][b] / like - first * first
        loglik_ref[b] = weight * jnp.log(like)
        one = jnp.sum(weight * first, axis=1, keepdims=True)
        two = jnp.sum(weight * second, axis=1, keepdims=True)
        share = jnp.where(lanes == b, one, share)
        share = jnp.where(lanes == branches + b, two, share)
    for d in range(share_ref.shape[0]):
        share_ref[d] = share


def block_likelihoods(aux, weight, operand, tiles, branches, states, devices):
    nblocks = operand.shape[0]
    vmem = pl.BlockSpec(memory_space=pltpu.VMEM)
    return pl.pallas_call(
        functools.partial(block_kernel, len(tiles), states),
        in_specs=[vmem] * (3 + len(tiles)),
        out_specs=[vmem] * 2,
        out_shape=[
            jax.ShapeDtypeStruct((branches, nblocks, BLK), F32),
            jax.ShapeDtypeStruct((devices, nblocks, BLK), F32),
        ],
        scratch_shapes=[pltpu.VMEM((branches, nblocks, BLK), F32)] * 3,
        name="blocks",
        compiler_params=LIMITS,
    )(aux, weight, operand, *tiles)


def sum_kernel(nblocks, branches, aux_ref, map_ref, lengths_ref, share_ref, part_ref, new_ref):
    owned = part_ref.shape[1]
    terms = part_ref.shape[0]
    share = share_ref[...]
    rows = share.shape[0]
    parts = lax.broadcasted_iota(jnp.int32, (rows, owned), 1) + lax.axis_index("dom") * owned
    ident = share[:, terms : terms + 1].astype(jnp.int32)
    onehot = (ident == parts).astype(F32)
    sums = lax.dot_general(
        share,
        onehot,
        (((0,), (0,)), ((), ())),
        precision=lax.Precision.HIGHEST,
        preferred_element_type=F32,
    )
    part_ref[...] = sums[:terms]
    total = jnp.sum(share, axis=0, keepdims=True)
    second = pltpu.roll(total, BLK - branches, 1)
    updated = aux_ref[pl.ds(2 * nblocks + branches, 1), :] - total / second
    lane = lax.broadcasted_iota(jnp.int32, (1, BLK), 1)
    place = map_ref[...]
    new = lengths_ref[...]
    for b in range(branches):
        value = jnp.sum(jnp.where(lane == b, updated, 0.0), axis=1, keepdims=True)
        new = jnp.where(place == b + 1, value, new)
    new_ref[...] = new


def add_up(aux, places, lengths, share, nblocks, branches, owned):
    vmem = pl.BlockSpec(memory_space=pltpu.VMEM)
    return pl.pallas_call(
        functools.partial(sum_kernel, nblocks, branches),
        in_specs=[vmem] * 4,
        out_specs=[vmem] * 2,
        out_shape=[
            jax.ShapeDtypeStruct((2 * branches, owned), F32),
            jax.ShapeDtypeStruct(lengths.shape, F32),
        ],
        name="sums",
        compiler_params=LIMITS,
    )(aux, places, lengths, share)


def on_device(
    top_partial,
    bottom_partial,
    left_vectors,
    right_vectors,
    decay_rates,
    state_weights,
    part_rates,
    branch_lengths,
    pattern_weights,
    block_partition,
    chosen_branches,
):
    branches, states, _, sites_here = top_partial.shape
    nblocks = sites_here // BLK
    owned = left_vectors.shape[0]
    groups = lax.axis_size("dom")
    pair = 2 if groups % 2 == 0 else 1
    rounds = groups // pair

    def shifted(value, r):
        step = [
            (d, ((d // pair + r) % rounds) * pair + d % pair) for d in range(groups)
        ]
        return lax.ppermute(value, "dom", step)

    blocks = block_partition[0]
    requests = [shifted(blocks, rounds - r) for r in range(1, rounds)]
    own = pack_tables(left_vectors, right_vectors, decay_rates, state_weights, part_rates)
    if pair == 2:
        partner = lax.ppermute(own, "dom", [(d, d ^ 1) for d in range(groups)])
    else:
        partner = own
    answers = [
        shifted(pick_tiles(request, own, partner, pair), r)
        for r, request in zip(range(1, rounds), requests)
    ]
    operand, tiles, aux, places = prepare(
        blocks,
        chosen_branches,
        branch_lengths,
        top_partial.reshape(branches * states * nblocks, BLK),
        bottom_partial.reshape(branches * states * nblocks, BLK),
        own,
        partner,
        states,
        pair,
        rounds,
    )
    tiles = [tiles] + answers[::-1]
    devices = lax.axis_size("site") * groups
    loglik, share = block_likelihoods(
        aux,
        pattern_weights.reshape(nblocks, BLK),
        operand,
        tiles,
        branches,
        states,
        devices,
    )
    everything = lax.all_to_all(
        share, ("site", "dom"), split_axis=0, concat_axis=0, tiled=True
    )
    count = branch_lengths.shape[0]
    rows = places.shape[0]
    padded = jnp.pad(branch_lengths, (0, rows * BLK - count)).reshape(rows, BLK)
    parts, new_lengths = add_up(
        aux,
        places,
        padded,
        everything.reshape(devices * nblocks, BLK),
        nblocks,
        branches,
        owned,
    )
    new_lengths = new_lengths.reshape(rows * BLK)[:count]
    return (
        loglik.reshape(branches, 1, sites_here),
        parts.reshape(2, branches, owned),
        new_lengths,
    )


def solution(mesh):
    return jax.shard_map(
        on_device,
        mesh=mesh,
        in_specs=(
            P(None, None, "dom", "site"),
            P(None, None, "dom", "site"),
            P("dom", None, None),
            P("dom", None, None),
            P("dom", None),
            P("dom", None),
            P("dom"),
            P(),
            P("dom", "site"),
            P("dom", "site"),
            P(),
        ),
        out_specs=(P(None, "dom", "site"), P(None, None, "dom"), P()),
        check_vma=False,
    )
```

```python
import functools

import jax
import jax.numpy as jnp
from jax import lax
from jax.experimental import pallas as pl
from jax.experimental.pallas import tpu as pltpu
from jax.sharding import PartitionSpec as P

BLK = 128
HALF = 64
SUB = 8
LOG2_E = 1.4426950408889634
F32 = jnp.float32
BF16 = jnp.bfloat16
LIMITS = pltpu.CompilerParams(vmem_limit_bytes=24 * 1024 * 1024)


def in_hbm(x):
    return pltpu.with_memory_space_constraint(x, pltpu.HBM)


def pack_kernel(
    rate_hbm,
    left_hbm,
    right_hbm,
    decay_hbm,
    weight_hbm,
    out_ref,
    rate_ref,
    left_ref,
    right_ref,
    decay_ref,
    weight_ref,
    small_sems,
    sems,
):
    chunks, states, group, _ = left_ref.shape
    small = [
        pltpu.make_async_copy(src, dst, small_sems.at[i])
        for i, (src, dst) in enumerate(
            ((rate_hbm, rate_ref), (decay_hbm, decay_ref), (weight_hbm, weight_ref))
        )
    ]
    for copy in small:
        copy.start()

    def copies(g):
        rows = pl.ds(g * group, group)
        return [
            pltpu.make_async_copy(src.at[:, rows, :], dst.at[g], sems.at[i, g])
            for i, (src, dst) in enumerate(((left_hbm, left_ref), (right_hbm, right_ref)))
        ]

    for g in range(chunks):
        for copy in copies(g):
            copy.start()
    for copy in small:
        copy.wait()
    left = left_ref.reshape(chunks * states * group, states)
    right = right_ref.reshape(chunks * states * group, states)
    for g in range(chunks):
        for copy in copies(g):
            copy.wait()
        for q in range(g * group, (g + 1) * group):
            rows_of = pl.ds(g * states * group + q - g * group, states, stride=group)
            table = left[rows_of, :]
            decay = decay_ref[pl.ds(q, 1), :]
            rows = jnp.concatenate(
                [table, decay, jnp.zeros((HALF - states - 1, states), F32)], axis=0
            )
            scale = jnp.concatenate(
                [
                    weight_ref[pl.ds(q, 1), :],
                    jnp.full((1, 1), -rate_ref[q], F32),
                    jnp.zeros((1, HALF - states - 1), F32),
                ],
                axis=1,
            )
            scaled = rows.T * scale
            other = right[rows_of, :]
            tile = jnp.concatenate(
                [scaled, other, jnp.zeros((states, HALF - states), F32)], axis=1
            )
            out_ref[q] = jnp.concatenate(
                [tile, jnp.zeros((HALF - states, 2 * HALF), F32)], axis=0
            )


def pack_tables(left, right, decay, weight, rate):
    parts, states, _ = left.shape
    group = 8
    chunks = parts // group
    hbm = pl.BlockSpec(memory_space=pltpu.HBM)
    table = pltpu.VMEM((chunks, states, group, states), F32)
    row = pltpu.VMEM((parts, states), F32)
    return pl.pallas_call(
        pack_kernel,
        in_specs=[hbm] * 5,
        out_specs=pl.BlockSpec(memory_space=pltpu.VMEM),
        out_shape=jax.ShapeDtypeStruct((parts, HALF, 2 * HALF), F32),
        scratch_shapes=[
            pltpu.SMEM((parts,), F32),
            table,
            table,
            row,
            row,
            pltpu.SemaphoreType.DMA((3,)),
            pltpu.SemaphoreType.DMA((2, chunks)),
        ],
        name="pack",
        compiler_params=LIMITS,
    )(
        in_hbm(rate),
        in_hbm(jnp.transpose(left, (1, 0, 2))),
        in_hbm(jnp.transpose(right, (1, 0, 2))),
        in_hbm(decay),
        in_hbm(weight),
    )


def copy_tiles(wanted_ref, own_ref, partner_ref, *out_refs):
    owned = own_ref.shape[0]
    base = lax.axis_index("dom") * owned
    place = 0
    for out_ref in out_refs:
        for n in range(out_ref.shape[0]):
            part = wanted_ref[place]
            row = lax.rem(part, owned)
            mine = part - row == base
            chosen = jnp.full((1, own_ref.shape[2]), mine.astype(jnp.int32))
            out_ref[n] = jnp.where(chosen == 1, own_ref[row], partner_ref[row])
            place += 1


def pick_tiles(wanted, own, partner, pieces):
    vmem = pl.BlockSpec(memory_space=pltpu.VMEM)
    count = wanted.shape[0] // pieces
    return pl.pallas_call(
        copy_tiles,
        in_specs=[pl.BlockSpec(memory_space=pltpu.SMEM), vmem, vmem],
        out_specs=[vmem] * pieces,
        out_shape=[jax.ShapeDtypeStruct((count,) + own.shape[1:], F32)] * pieces,
        name="pick",
        compiler_params=LIMITS,
    )(wanted, own, partner)


def prepare_kernel(
    pair,
    rounds,
    blocks_ref,
    chosen_ref,
    lengths_ref,
    padded_ref,
    top_hbm,
    bottom_hbm,
    own_ref,
    partner_ref,
    out_ref,
    tiles_ref,
    aux_ref,
    map_ref,
    rows_ref,
    top_ref,
    bottom_ref,
    sems,
):
    nblocks = out_ref.shape[0]
    chunks = sems.shape[1]
    chunk = top_ref.shape[0] // chunks
    columns = out_ref.shape[3] // chunks
    fused = columns // BLK
    states = chunk // (fused * nblocks)
    branches = chosen_ref.shape[0]

    def copies(g):
        rows = pl.ds(g * chunk, chunk)
        return [
            pltpu.make_async_copy(src.at[rows], dst.at[rows], sems.at[i, g])
            for i, (src, dst) in enumerate(((top_hbm, top_ref), (bottom_hbm, bottom_ref)))
        ]

    for g in range(chunks):
        for copy in copies(g):
            copy.start()
    copy_tiles(blocks_ref, own_ref, partner_ref, tiles_ref)
    owned = own_ref.shape[0]
    my_pair = lax.axis_index("dom") // pair
    lane = lax.broadcasted_iota(jnp.int32, (1, BLK), 1)
    flat = lax.broadcasted_iota(jnp.int32, map_ref.shape, 0) * BLK
    flat = flat + lax.broadcasted_iota(jnp.int32, map_ref.shape, 1)
    for n in range(nblocks):
        part = blocks_ref[n]
        distance = lax.rem(lax.div(part, owned * pair) - my_pair + rounds, rounds)
        aux_ref[pl.ds(n, 1), :] = jnp.full((1, BLK), distance.astype(F32), F32)
        aux_ref[pl.ds(nblocks + n, 1), :] = jnp.full((1, BLK), part.astype(F32), F32)
    along = jnp.zeros((1, BLK), F32)
    update = jnp.zeros(map_ref.shape, jnp.int32)
    for b in range(branches):
        place = chosen_ref[b]
        time = lengths_ref[place]
        aux_ref[pl.ds(2 * nblocks + 8 + b, 1), :] = jnp.full((1, BLK), time, F32)
        along = jnp.where(lane == b, time, along)
        update = jnp.where(flat == place, b + 1, update)
    aux_ref[pl.ds(2 * nblocks, 1), :] = along
    map_ref[...] = update
    rows_ref[...] = padded_ref[...]
    pad = jnp.zeros((HALF - states, BLK), F32)

    def step(g, carry):
        for copy in copies(g):
            copy.wait()
        for b in range(fused):
            for n in range(nblocks):
                for side, ref in enumerate((top_ref, bottom_ref)):
                    first = g * chunk + b * states * nblocks + n
                    rows = ref[pl.ds(first, states, stride=nblocks), :]
                    full = jnp.concatenate([rows, pad], axis=0)
                    high = full.astype(BF16)
                    low = (full - high.astype(F32)).astype(BF16)
                    lanes = pl.ds(pl.multiple_of(g * columns + b * BLK, BLK), BLK)
                    out_ref[n, side, pl.ds(0, HALF), lanes] = high
                    out_ref[n, side, pl.ds(HALF, HALF), lanes] = low
        return carry

    lax.fori_loop(0, chunks, step, 0)


def prepare(blocks, chosen, lengths, padded, top, bottom, own, partner, states, pair, rounds):
    nblocks = blocks.shape[0]
    branches = chosen.shape[0]
    chunks = branches // 2
    smem = pl.BlockSpec(memory_space=pltpu.SMEM)
    hbm = pl.BlockSpec(memory_space=pltpu.HBM)
    vmem = pl.BlockSpec(memory_space=pltpu.VMEM)
    return pl.pallas_call(
        functools.partial(prepare_kernel, pair, rounds),
        in_specs=[smem, smem, smem, vmem, hbm, hbm, vmem, vmem],
        out_specs=[vmem] * 5,
        out_shape=[
            jax.ShapeDtypeStruct((nblocks, 2, 2 * HALF, branches * BLK), BF16),
            jax.ShapeDtypeStruct((nblocks,) + own.shape[1:], F32),
            jax.ShapeDtypeStruct((2 * nblocks + 8 + branches, BLK), F32),
            jax.ShapeDtypeStruct(padded.shape, jnp.int32),
            jax.ShapeDtypeStruct(padded.shape, F32),
        ],
        scratch_shapes=[
            pltpu.VMEM(top.shape, F32),
            pltpu.VMEM(top.shape, F32),
            pltpu.SemaphoreType.DMA((2, chunks)),
        ],
        name="prepare",
        compiler_params=LIMITS,
    )(blocks, chosen, lengths, padded, in_hbm(top), in_hbm(bottom), own, partner)


def block_kernel(rounds, states, pieces, piece, aux_ref, weight_ref, operand_ref, own_ref, *refs):
    tiles = refs[: rounds - 1]
    earlier = refs[rounds - 1 : rounds - 1 + (piece if piece == pieces - 1 else 0)]
    like_ref, terms_ref, partial_ref = refs[-3:]
    branches, count, _ = like_ref.shape
    nblocks = operand_ref.shape[0]
    start = piece * count
    wide = 2 * BLK
    lane = lax.broadcasted_iota(jnp.int32, (HALF, 2 * HALF), 1)
    is_left = lane < HALF
    for m in range(count):
        n = start + m
        distance = aux_ref[pl.ds(n, 1), :]
        tile = own_ref[n]
        for r in range(1, rounds):
            tile = jnp.where(distance == float(r), tiles[r - 1][m], tile)
        turned = pltpu.roll(tile, HALF, 1)
        sides = []
        for double in (jnp.where(is_left, tile, turned), jnp.where(is_left, turned, tile)):
            high = double.astype(BF16)
            low = (double - high.astype(F32)).astype(BF16)
            sides.append(jnp.concatenate([high, low[:, :HALF]], axis=1))
        expo = jnp.broadcast_to(tile[:, states : states + 1], (HALF, BLK))
        scaled = expo * LOG2_E
        for c in range(branches * BLK // wide):
            columns = pl.ds(c * wide, wide)
            prods = []
            for side, lhs in enumerate(sides):
                part = operand_ref[n, side, :, columns]
                rhs = jnp.concatenate([part, part[:HALF]], axis=0)
                prods.append(jnp.dot(lhs, rhs, preferred_element_type=F32))
            joint = prods[0] * prods[1]
            for h in range(wide // BLK):
                b = c * (wide // BLK) + h
                time = aux_ref[pl.ds(2 * nblocks + 8 + b, 1), :]
                zeroth = joint[:, h * BLK : (h + 1) * BLK] * jnp.exp2(scaled * time)
                first = zeroth * expo
                second = first * expo
                for i, term in enumerate((zeroth, first, second)):
                    total = term[:SUB]
                    for k in range(SUB, HALF, SUB):
                        total = total + term[k : k + SUB]
                    partial_ref[i, b, pl.ds(m * SUB, SUB), :] = total

    weight = weight_ref[pl.ds(start, count), :].astype(F32)
    lanes = lax.broadcasted_iota(jnp.int32, (count, BLK), 1)
    terms = jnp.where(lanes == 2 * branches, aux_ref[pl.ds(nblocks + start, count), :], 0.0)
    for b in range(branches):
        sums = []
        for i in range(3):
            total = partial_ref[i, b, pl.ds(0, count, stride=SUB), :]
            for j in range(1, SUB):
                total = total + partial_ref[i, b, pl.ds(j, count, stride=SUB), :]
            sums.append(total)
        like_ref[b] = sums[0]
        inverse = 1.0 / sums[0]
        first = sums[1] * inverse
        second = sums[2] * inverse - first * first
        one = jnp.sum(weight * first, axis=1, keepdims=True)
        two = jnp.sum(weight * second, axis=1, keepdims=True)
        terms = jnp.where(lanes == b, one, terms)
        terms = jnp.where(lanes == branches + b, two, terms)
    if piece < pieces - 1:
        terms_ref[...] = terms
    else:
        for ref in earlier:
            terms = ref[...] + pltpu.roll(terms, HALF, 1)
        for d in range(terms_ref.shape[0]):
            terms_ref[d] = terms


def block_likelihoods(
    aux, weight, operand, own_tiles, tiles, earlier, branches, states, devices, pieces, piece
):
    nblocks = operand.shape[0]
    count = nblocks // pieces
    vmem = pl.BlockSpec(memory_space=pltpu.VMEM)
    last = piece == pieces - 1
    return pl.pallas_call(
        functools.partial(block_kernel, len(tiles) + 1, states, pieces, piece),
        in_specs=[vmem] * (4 + len(tiles) + len(earlier)),
        out_specs=[vmem] * 2,
        out_shape=[
            jax.ShapeDtypeStruct((branches, count, BLK), F32),
            jax.ShapeDtypeStruct(((devices,) if last else ()) + (count, BLK), F32),
        ],
        scratch_shapes=[pltpu.VMEM((3, branches, count * SUB, BLK), F32)],
        name="blocks",
        compiler_params=LIMITS,
    )(aux, weight, operand, own_tiles, *tiles, *earlier)


def sum_kernel(aux_ref, map_ref, lengths_ref, weight_ref, share_ref, *refs):
    like_refs = refs[:-3]
    part_ref, new_ref, loglik_ref = refs[-3:]
    branches, count, _ = like_refs[0].shape
    nblocks = count * len(like_refs)
    owned = part_ref.shape[1]
    terms = part_ref.shape[0]
    share = share_ref[...]
    if len(like_refs) > 1:
        share = jnp.concatenate([share, pltpu.roll(share, HALF, 1)], axis=0)
    share = share[:, :HALF]
    parts = lax.broadcasted_iota(jnp.int32, (share.shape[0], owned), 1)
    parts = parts + lax.axis_index("dom") * owned
    ident = share[:, terms : terms + 1].astype(jnp.int32)
    onehot = (ident == parts).astype(F32)
    sums = lax.dot_general(
        share,
        onehot,
        (((0,), (0,)), ((), ())),
        precision=lax.Precision.HIGHEST,
        preferred_element_type=F32,
    )
    part_ref[...] = sums[:terms]
    total = jnp.sum(share, axis=0, keepdims=True)
    total = jnp.concatenate([total, total], axis=1)
    second = pltpu.roll(total, BLK - branches, 1)
    updated = aux_ref[pl.ds(2 * nblocks, 1), :] - total / second
    lane = lax.broadcasted_iota(jnp.int32, (1, BLK), 1)
    place = map_ref[...]
    new = lengths_ref[...]
    for b in range(branches):
        value = jnp.sum(jnp.where(lane == b, updated, 0.0), axis=1, keepdims=True)
        new = jnp.where(place == b + 1, value, new)
    new_ref[...] = new
    for i, like_ref in enumerate(like_refs):
        blocks = pl.ds(i * count, count)
        weight = weight_ref[blocks, :].astype(F32)
        for b in range(branches):
            loglik_ref[b, blocks, :] = weight * jnp.log(like_ref[b])


def add_up(aux, places, lengths, weight, share, likes, owned):
    vmem = pl.BlockSpec(memory_space=pltpu.VMEM)
    branches = likes[0].shape[0]
    nblocks = weight.shape[0]
    return pl.pallas_call(
        sum_kernel,
        in_specs=[vmem] * (5 + len(likes)),
        out_specs=[vmem] * 3,
        out_shape=[
            jax.ShapeDtypeStruct((2 * branches, owned), F32),
            jax.ShapeDtypeStruct(lengths.shape, F32),
            jax.ShapeDtypeStruct((branches, nblocks, BLK), F32),
        ],
        name="sums",
        compiler_params=LIMITS,
    )(aux, places, lengths, weight, share, *likes)


def on_device(
    top_partial,
    bottom_partial,
    left_vectors,
    right_vectors,
    decay_rates,
    state_weights,
    part_rates,
    branch_lengths,
    pattern_weights,
    block_partition,
    chosen_branches,
):
    branches, states, _, sites_here = top_partial.shape
    nblocks = sites_here // BLK
    owned = left_vectors.shape[0]
    groups = lax.axis_size("dom")
    pair = 2 if groups % 2 == 0 else 1
    rounds = groups // pair

    def shifted(value, r):
        step = [
            (d, ((d // pair + r) % rounds) * pair + d % pair) for d in range(groups)
        ]
        return lax.ppermute(value, "dom", step)

    blocks = block_partition[0]
    requests = [shifted(blocks, rounds - r) for r in range(1, rounds)]
    own = pack_tables(left_vectors, right_vectors, decay_rates, state_weights, part_rates)
    if pair == 2:
        partner = lax.ppermute(own, "dom", [(d, d ^ 1) for d in range(groups)])
    else:
        partner = own
    pieces = 2 if nblocks % 2 == 0 else 1
    answers = []
    for r, request in zip(range(1, rounds), requests):
        answers.append([shifted(t, r) for t in pick_tiles(request, own, partner, pieces)])
    count = branch_lengths.shape[0]
    rows = -(-count // BLK)
    padded = jnp.pad(branch_lengths, (0, rows * BLK - count)).reshape(rows, BLK)
    operand, tiles, aux, places, lengths = prepare(
        blocks,
        chosen_branches,
        branch_lengths,
        padded,
        top_partial.reshape(branches * states * nblocks, BLK),
        bottom_partial.reshape(branches * states * nblocks, BLK),
        own,
        partner,
        states,
        pair,
        rounds,
    )
    answers = answers[::-1]
    devices = lax.axis_size("site") * groups
    weight = pattern_weights.reshape(nblocks, BLK)
    likes, earlier = [], []
    for piece in range(pieces):
        like, terms = block_likelihoods(
            aux,
            weight,
            operand,
            tiles,
            [answer[piece] for answer in answers],
            earlier,
            branches,
            states,
            devices,
            pieces,
            piece,
        )
        likes.append(like)
        earlier = [terms]
    everything = lax.all_to_all(
        terms, ("site", "dom"), split_axis=0, concat_axis=0, tiled=True
    )
    parts, new_lengths, loglik = add_up(
        aux, places, lengths, weight, everything.reshape(-1, BLK), likes, owned
    )
    new_lengths = new_lengths.reshape(rows * BLK)[:count]
    return (
        loglik.reshape(branches, 1, sites_here),
        parts.reshape(2, branches, owned),
        new_lengths,
    )


def solution(mesh):
    return jax.shard_map(
        on_device,
        mesh=mesh,
        in_specs=(
            P(None, None, "dom", "site"),
            P(None, None, "dom", "site"),
            P("dom", None, None),
            P("dom", None, None),
            P("dom", None),
            P("dom", None),
            P("dom"),
            P(),
            P("dom", "site"),
            P("dom", "site"),
            P(),
        ),
        out_specs=(P(None, "dom", "site"), P(None, None, "dom"), P()),
        check_vma=False,
    )
```

```python
import functools

import jax
import jax.numpy as jnp
from jax import lax
from jax.experimental import pallas as pl
from jax.experimental.pallas import tpu as pltpu
from jax.sharding import PartitionSpec as P


BLK = 128
HALF = 64
SUB = 8
EARLY = 6
LOG2_E = 1.4426950408889634
F32 = jnp.float32
BF16 = jnp.bfloat16
LIMITS = pltpu.CompilerParams(vmem_limit_bytes=24 * 1024 * 1024)


def in_hbm(x):
    return pltpu.with_memory_space_constraint(x, pltpu.HBM)


def pack_kernel(
    rate_hbm,
    left_hbm,
    right_hbm,
    decay_hbm,
    weight_hbm,
    out_ref,
    right_ref,
    rate_ref,
    left_ref,
    decay_ref,
    weight_ref,
    small_sems,
    sems,
    right_sem,
):
    chunks, states, group, _ = left_ref.shape
    half = out_ref.shape[0]
    small = [
        pltpu.make_async_copy(src, dst, small_sems.at[i])
        for i, (src, dst) in enumerate(
            ((rate_hbm, rate_ref), (decay_hbm, decay_ref), (weight_hbm, weight_ref))
        )
    ]
    for copy in small:
        copy.start()

    def chunk_copy(g):
        rows = pl.ds(g * group, group)
        return pltpu.make_async_copy(left_hbm.at[:, rows, :], left_ref.at[g], sems.at[g])

    for g in range(chunks // 2):
        chunk_copy(g).start()
        chunk_copy(g + chunks // 2).start()
    right_copy = pltpu.make_async_copy(right_hbm, right_ref, right_sem)
    right_copy.start()
    for copy in small:
        copy.wait()
    left = left_ref.reshape(chunks * states * group, states)
    gap = jnp.zeros((states, HALF - states), F32)

    def beside(first, second):
        space = gap[: first.shape[0]]
        return jnp.concatenate([first, space, second, space], axis=1)

    def exponents(q):
        return -(decay_ref[pl.ds(q, 1), :] * rate_ref[q])

    for g in range(chunks // 2):
        chunk_copy(g).wait()
        chunk_copy(g + chunks // 2).wait()
        for i in range(group):
            q = g * group + i
            tables = [
                left[pl.ds(c * states * group + i, states, stride=group), :]
                for c in (g, g + chunks // 2)
            ]
            out_ref[q, pl.ds(0, states), :] = beside(*tables)
            out_ref[q, pl.ds(states, 1), :] = beside(exponents(q), exponents(q + half))
            out_ref[q, pl.ds(states + 1, 1), :] = beside(
                weight_ref[pl.ds(q, 1), :], weight_ref[pl.ds(q + half, 1), :]
            )
            rest = HALF - states - 2
            out_ref[q, pl.ds(states + 2, rest), :] = jnp.zeros((rest, 2 * HALF), F32)
    right_copy.wait()


def pack_tables(left, right, decay, weight, rate):
    states, parts, _ = left.shape
    group = 8
    chunks = parts // group
    hbm = pl.BlockSpec(memory_space=pltpu.HBM)
    row = pltpu.VMEM((parts, states), F32)
    return pl.pallas_call(
        pack_kernel,
        in_specs=[hbm] * 5,
        out_specs=[pl.BlockSpec(memory_space=pltpu.VMEM)] * 2,
        out_shape=[
            jax.ShapeDtypeStruct((parts // 2, HALF, 2 * HALF), F32),
            jax.ShapeDtypeStruct(right.shape, F32),
        ],
        scratch_shapes=[
            pltpu.SMEM((parts,), F32),
            pltpu.VMEM((chunks, states, group, states), F32),
            row,
            row,
            pltpu.SemaphoreType.DMA((3,)),
            pltpu.SemaphoreType.DMA((chunks,)),
            pltpu.SemaphoreType.DMA,
        ],
        name="pack",
        compiler_params=LIMITS,
    )(in_hbm(rate), in_hbm(left), in_hbm(right), in_hbm(decay), in_hbm(weight))


def copy_tiles(wanted_ref, own_left, own_right, partner_left, partner_right, *out_refs):
    states, owned, _ = own_right.shape
    half = own_left.shape[0]
    base = lax.axis_index("dom") * owned
    rights = [ref.reshape(states * owned, states) for ref in (own_right, partner_right)]
    lane = lax.broadcasted_iota(jnp.int32, (HALF, 2 * HALF), 1)
    is_left = lane < HALF
    gap = jnp.zeros((states, 2 * HALF - states), F32)
    below = jnp.zeros((HALF - states, 2 * HALF), F32)
    place = 0
    for out_ref in out_refs:
        for n in range(out_ref.shape[0]):
            part = wanted_ref[place]
            row = lax.rem(part, owned)
            mine = part - row == base

            def chosen(flag):
                return jnp.full((1, 2 * HALF), flag.astype(jnp.int32)) == 1

            second = row >= half
            at = jnp.where(second, row - half, row)
            left = jnp.where(chosen(mine), own_left[at], partner_left[at])
            left = jnp.where(chosen(second), pltpu.roll(left, HALF, 1), left)
            table = [ref[pl.ds(row, states, stride=owned), :] for ref in rights]
            right = jnp.where(chosen(mine)[:, :states], *table)
            right = jnp.concatenate([jnp.concatenate([right, gap], axis=1), below], axis=0)
            out_ref[n] = jnp.where(is_left, left, pltpu.roll(right, HALF, 1))
            place += 1


def pick_tiles(wanted, tables, pieces):
    vmem = pl.BlockSpec(memory_space=pltpu.VMEM)
    count = wanted.shape[0] // pieces
    return pl.pallas_call(
        copy_tiles,
        in_specs=[pl.BlockSpec(memory_space=pltpu.SMEM)] + [vmem] * 4,
        out_specs=[vmem] * pieces,
        out_shape=[jax.ShapeDtypeStruct((count, HALF, 2 * HALF), F32)] * pieces,
        name="pick",
        compiler_params=LIMITS,
    )(wanted, *tables)


def start_split(skip, top_hbm, bottom_hbm, top_ref, bottom_ref, sems):
    chunks = sems.shape[1]
    chunk = top_ref.shape[0] // chunks

    def copies(g):
        there = pl.ds(g * chunk, chunk)
        here = pl.ds((skip + g) * chunk, chunk)
        return [
            pltpu.make_async_copy(src.at[here], dst.at[there], sems.at[i, g])
            for i, (src, dst) in enumerate(((top_hbm, top_ref), (bottom_hbm, bottom_ref)))
        ]

    for g in range(chunks):
        for copy in copies(g):
            copy.start()
    return copies


def finish_split(copies, out_ref, top_ref, bottom_ref, sems):
    nblocks = out_ref.shape[0]
    chunks = sems.shape[1]
    chunk = top_ref.shape[0] // chunks
    columns = out_ref.shape[3] // chunks
    fused = columns // BLK
    states = chunk // (fused * nblocks)
    pad = jnp.zeros((HALF - states, BLK), F32)

    def step(g, carry):
        for copy in copies(g):
            copy.wait()
        for b in range(fused):
            for n in range(nblocks):
                for side, ref in enumerate((top_ref, bottom_ref)):
                    first = g * chunk + b * states * nblocks + n
                    rows = ref[pl.ds(first, states, stride=nblocks), :]
                    full = jnp.concatenate([rows, pad], axis=0)
                    high = full.astype(BF16)
                    low = (full - high.astype(F32)).astype(BF16)
                    lanes = pl.ds(pl.multiple_of(g * columns + b * BLK, BLK), BLK)
                    out_ref[n, side, pl.ds(0, HALF), lanes] = high
                    out_ref[n, side, pl.ds(HALF, HALF), lanes] = low
        return carry

    lax.fori_loop(0, chunks, step, 0)


def early_kernel(top_hbm, bottom_hbm, out_ref, top_ref, bottom_ref, sems):
    copies = start_split(0, top_hbm, bottom_hbm, top_ref, bottom_ref, sems)
    finish_split(copies, out_ref, top_ref, bottom_ref, sems)


def late_kernel(
    skip,
    pair,
    rounds,
    blocks_ref,
    chosen_ref,
    lengths_ref,
    padded_ref,
    top_hbm,
    bottom_hbm,
    own_left,
    own_right,
    partner_left,
    partner_right,
    out_ref,
    tiles_ref,
    aux_ref,
    map_ref,
    rows_ref,
    top_ref,
    bottom_ref,
    sems,
):
    nblocks = out_ref.shape[0]
    branches = chosen_ref.shape[0]
    owned = own_right.shape[1]
    copies = start_split(skip, top_hbm, bottom_hbm, top_ref, bottom_ref, sems)
    copy_tiles(blocks_ref, own_left, own_right, partner_left, partner_right, tiles_ref)
    my_pair = lax.axis_index("dom") // pair
    lane = lax.broadcasted_iota(jnp.int32, (1, BLK), 1)
    flat = lax.broadcasted_iota(jnp.int32, map_ref.shape, 0) * BLK
    flat = flat + lax.broadcasted_iota(jnp.int32, map_ref.shape, 1)
    for n in range(nblocks):
        part = blocks_ref[n]
        distance = lax.rem(lax.div(part, owned * pair) - my_pair + rounds, rounds)
        aux_ref[pl.ds(n, 1), :] = jnp.full((1, BLK), distance.astype(F32), F32)
        aux_ref[pl.ds(nblocks + n, 1), :] = jnp.full((1, BLK), part.astype(F32), F32)
    along = jnp.zeros((1, BLK), F32)
    update = jnp.zeros(map_ref.shape, jnp.int32)
    for b in range(branches):
        place = chosen_ref[b]
        time = lengths_ref[place]
        aux_ref[pl.ds(2 * nblocks + 8 + b, 1), :] = jnp.full((1, BLK), time, F32)
        along = jnp.where(lane == b, time, along)
        update = jnp.where(flat == place, b + 1, update)
    aux_ref[pl.ds(2 * nblocks, 1), :] = along
    map_ref[...] = update
    rows_ref[...] = padded_ref[...]
    finish_split(copies, out_ref, top_ref, bottom_ref, sems)


def split_scratch(top, branches, taken, fused):
    rows = top.shape[0] // branches * taken
    return [
        pltpu.VMEM((rows, BLK), F32),
        pltpu.VMEM((rows, BLK), F32),
        pltpu.SemaphoreType.DMA((2, taken // fused)),
    ]


def prepare_early(top, bottom, nblocks, branches, taken):
    hbm = pl.BlockSpec(memory_space=pltpu.HBM)
    return pl.pallas_call(
        early_kernel,
        in_specs=[hbm, hbm],
        out_specs=pl.BlockSpec(memory_space=pltpu.VMEM),
        out_shape=jax.ShapeDtypeStruct((nblocks, 2, 2 * HALF, taken * BLK), BF16),
        scratch_shapes=split_scratch(top, branches, taken, 2),
        name="early",
        compiler_params=LIMITS,
    )(in_hbm(top), in_hbm(bottom))


def prepare_late(
    blocks, chosen, lengths, padded, top, bottom, tables, skipped, pair, rounds
):
    nblocks = blocks.shape[0]
    branches = chosen.shape[0]
    taken = branches - skipped
    smem = pl.BlockSpec(memory_space=pltpu.SMEM)
    hbm = pl.BlockSpec(memory_space=pltpu.HBM)
    vmem = pl.BlockSpec(memory_space=pltpu.VMEM)
    return pl.pallas_call(
        functools.partial(late_kernel, skipped // 2, pair, rounds),
        in_specs=[smem, smem, smem, vmem, hbm, hbm] + [vmem] * 4,
        out_specs=[vmem] * 5,
        out_shape=[
            jax.ShapeDtypeStruct((nblocks, 2, 2 * HALF, taken * BLK), BF16),
            jax.ShapeDtypeStruct((nblocks, HALF, 2 * HALF), F32),
            jax.ShapeDtypeStruct((2 * nblocks + 8 + branches, BLK), F32),
            jax.ShapeDtypeStruct(padded.shape, jnp.int32),
            jax.ShapeDtypeStruct(padded.shape, F32),
        ],
        scratch_shapes=split_scratch(top, branches, taken, 2),
        name="late",
        compiler_params=LIMITS,
    )(blocks, chosen, lengths, padded, in_hbm(top), in_hbm(bottom), *tables)


def block_kernel(rounds, states, pieces, piece, aux_ref, weight_ref, early_ref, late_ref, own_ref, *refs):
    tiles = refs[: rounds - 1]
    earlier = refs[rounds - 1 : rounds - 1 + (piece if piece == pieces - 1 else 0)]
    like_ref, terms_ref, partial_ref = refs[-3:]
    branches, count, _ = like_ref.shape
    nblocks = early_ref.shape[0]
    split = early_ref.shape[3]
    start = piece * count
    wide = 2 * BLK
    lane = lax.broadcasted_iota(jnp.int32, (HALF, 2 * HALF), 1)
    is_left = lane < HALF
    for m in range(count):
        n = start + m
        distance = aux_ref[pl.ds(n, 1), :]
        tile = own_ref[n]
        for r in range(1, rounds):
            tile = jnp.where(distance == float(r), tiles[r - 1][m], tile)
        turned = pltpu.roll(tile, HALF, 1)
        flipped = tile[:, :HALF].T
        scaled = flipped * tile[states + 1 : states + 2, :HALF]
        left = jnp.concatenate([scaled, scaled], axis=1)
        sides = []
        for double in (left, jnp.where(is_left, turned, tile)):
            high = double.astype(BF16)
            low = (double - high.astype(F32)).astype(BF16)
            sides.append(jnp.concatenate([high, low[:, :HALF]], axis=1))
        expo = jnp.broadcast_to(flipped[:, states : states + 1], (HALF, BLK))
        powers = expo * LOG2_E
        for c in range(branches * BLK // wide):
            prods = []
            for side, lhs in enumerate(sides):
                if c * wide < split:
                    part = early_ref[n, side, :, pl.ds(c * wide, wide)]
                else:
                    part = late_ref[n, side, :, pl.ds(c * wide - split, wide)]
                rhs = jnp.concatenate([part, part[:HALF]], axis=0)
                prods.append(jnp.dot(lhs, rhs, preferred_element_type=F32))
            joint = prods[0] * prods[1]
            for h in range(wide // BLK):
                b = c * (wide // BLK) + h
                time = aux_ref[pl.ds(2 * nblocks + 8 + b, 1), :]
                zeroth = joint[:, h * BLK : (h + 1) * BLK] * jnp.exp2(powers * time)
                first = zeroth * expo
                second = first * expo
                for i, term in enumerate((zeroth, first, second)):
                    total = term[:SUB]
                    for k in range(SUB, HALF, SUB):
                        total = total + term[k : k + SUB]
                    partial_ref[i, b, pl.ds(m * SUB, SUB), :] = total

    weight = weight_ref[pl.ds(start, count), :].astype(F32)
    lanes = lax.broadcasted_iota(jnp.int32, (count, BLK), 1)
    terms = jnp.where(lanes == 2 * branches, aux_ref[pl.ds(nblocks + start, count), :], 0.0)
    for b in range(branches):
        sums = []
        for i in range(3):
            total = partial_ref[i, b, pl.ds(0, count, stride=SUB), :]
            for j in range(1, SUB):
                total = total + partial_ref[i, b, pl.ds(j, count, stride=SUB), :]
            sums.append(total)
        like_ref[b] = sums[0]
        inverse = 1.0 / sums[0]
        first = sums[1] * inverse
        second = sums[2] * inverse - first * first
        one = jnp.sum(weight * first, axis=1, keepdims=True)
        two = jnp.sum(weight * second, axis=1, keepdims=True)
        terms = jnp.where(lanes == b, one, terms)
        terms = jnp.where(lanes == branches + b, two, terms)
    if piece < pieces - 1:
        terms_ref[...] = terms
    else:
        terms = [ref[...] for ref in earlier] + [terms]
        for d in range(terms_ref.shape[0]):
            for i in range(0, pieces, 2):
                pair = terms[i] + pltpu.roll(terms[i + 1], HALF, 1)
                terms_ref[d, pl.ds(i // 2 * count, count), :] = pair


def block_likelihoods(
    aux, weight, operands, own_tiles, tiles, earlier, branches, states, devices, pieces, piece
):
    nblocks = operands[0].shape[0]
    count = nblocks // pieces
    vmem = pl.BlockSpec(memory_space=pltpu.VMEM)
    last = piece == pieces - 1
    return pl.pallas_call(
        functools.partial(block_kernel, len(tiles) + 1, states, pieces, piece),
        in_specs=[vmem] * (5 + len(tiles) + len(earlier)),
        out_specs=[vmem] * 2,
        out_shape=[
            jax.ShapeDtypeStruct((branches, count, BLK), F32),
            jax.ShapeDtypeStruct((devices, nblocks // 2, BLK) if last else (count, BLK), F32),
        ],
        scratch_shapes=[pltpu.VMEM((3, branches, count * SUB, BLK), F32)],
        name="blocks",
        compiler_params=LIMITS,
    )(aux, weight, *operands, own_tiles, *tiles, *earlier)


def sum_kernel(aux_ref, map_ref, lengths_ref, weight_ref, share_ref, *refs):
    like_refs = refs[:-3]
    part_ref, new_ref, loglik_ref = refs[-3:]
    branches, count, _ = like_refs[0].shape
    nblocks = count * len(like_refs)
    owned = part_ref.shape[1]
    terms = part_ref.shape[0]
    share = share_ref[...]
    share = jnp.concatenate([share, pltpu.roll(share, HALF, 1)], axis=0)
    share = share[:, :HALF]
    parts = lax.broadcasted_iota(jnp.int32, (share.shape[0], owned), 1)
    parts = parts + lax.axis_index("dom") * owned
    ident = share[:, terms : terms + 1].astype(jnp.int32)
    onehot = (ident == parts).astype(F32)
    sums = lax.dot_general(
        share,
        onehot,
        (((0,), (0,)), ((), ())),
        precision=lax.Precision.HIGHEST,
        preferred_element_type=F32,
    )
    part_ref[...] = sums[:terms]
    total = jnp.sum(share, axis=0, keepdims=True)
    total = jnp.concatenate([total, total], axis=1)
    second = pltpu.roll(total, BLK - branches, 1)
    updated = aux_ref[pl.ds(2 * nblocks, 1), :] - total / second
    lane = lax.broadcasted_iota(jnp.int32, (1, BLK), 1)
    place = map_ref[...]
    new = lengths_ref[...]
    for b in range(branches):
        value = jnp.sum(jnp.where(lane == b, updated, 0.0), axis=1, keepdims=True)
        new = jnp.where(place == b + 1, value, new)
    new_ref[...] = new
    for i, like_ref in enumerate(like_refs):
        blocks = pl.ds(i * count, count)
        weight = weight_ref[blocks, :].astype(F32)
        for b in range(branches):
            loglik_ref[b, blocks, :] = weight * jnp.log(like_ref[b])


def add_up(aux, places, lengths, weight, share, likes, owned):
    vmem = pl.BlockSpec(memory_space=pltpu.VMEM)
    branches = likes[0].shape[0]
    nblocks = weight.shape[0]
    return pl.pallas_call(
        sum_kernel,
        in_specs=[vmem] * (5 + len(likes)),
        out_specs=[vmem] * 3,
        out_shape=[
            jax.ShapeDtypeStruct((2 * branches, owned), F32),
            jax.ShapeDtypeStruct(lengths.shape, F32),
            jax.ShapeDtypeStruct((branches, nblocks, BLK), F32),
        ],
        name="sums",
        compiler_params=LIMITS,
    )(aux, places, lengths, weight, share, *likes)


def compute(
    top_partial,
    bottom_partial,
    left_vectors,
    right_vectors,
    decay_rates,
    state_weights,
    part_rates,
    branch_lengths,
    pattern_weights,
    block_partition,
    chosen_branches,
):
    branches, states, _, sites_here = top_partial.shape
    nblocks = sites_here // BLK
    owned = left_vectors.shape[0]
    groups = lax.axis_size("dom")
    pair = 2 if groups % 2 == 0 else 1
    rounds = groups // pair

    def shifted(value, r):
        step = [
            (d, ((d // pair + r) % rounds) * pair + d % pair) for d in range(groups)
        ]
        return lax.ppermute(value, "dom", step)

    blocks = block_partition[0]
    requests = [shifted(blocks, rounds - r) for r in range(1, rounds)]
    left_turned = jnp.transpose(left_vectors, (1, 0, 2))
    right_turned = jnp.transpose(right_vectors, (1, 0, 2))

    def swapped(value):
        if pair == 1:
            return value
        return lax.ppermute(value, "dom", [(d, d ^ 1) for d in range(groups)])

    partner_right = swapped(right_turned)
    own = pack_tables(left_turned, right_turned, decay_rates, state_weights, part_rates)
    partner_left = swapped(own[0])
    tables = [*own, partner_left, partner_right]
    pieces = 2
    answers = []
    for r, request in zip(range(1, rounds), requests):
        answers.append([shifted(t, r) for t in pick_tiles(request, tables, pieces)])
    count = branch_lengths.shape[0]
    rows = -(-count // BLK)
    padded = jnp.pad(branch_lengths, (0, rows * BLK - count)).reshape(rows, BLK)
    top = top_partial.reshape(branches * states * nblocks, BLK)
    bottom = bottom_partial.reshape(branches * states * nblocks, BLK)
    early = prepare_early(top, bottom, nblocks, branches, EARLY)
    late, tiles, aux, places, lengths = prepare_late(
        blocks,
        chosen_branches,
        branch_lengths,
        padded,
        top,
        bottom,
        tables,
        EARLY,
        pair,
        rounds,
    )
    operands = [early, late]
    answers = answers[::-1]
    devices = lax.axis_size("site") * groups
    weight = pattern_weights.reshape(nblocks, BLK)
    likes, earlier = [], []
    for piece in range(pieces):
        like, terms = block_likelihoods(
            aux,
            weight,
            operands,
            tiles,
            [answer[piece] for answer in answers],
            earlier,
            branches,
            states,
            devices,
            pieces,
            piece,
        )
        likes.append(like)
        earlier.append(terms)
    everything = lax.all_to_all(
        terms, ("site", "dom"), split_axis=0, concat_axis=0, tiled=True
    )
    parts, new_lengths, loglik = add_up(
        aux, places, lengths, weight, everything.reshape(-1, BLK), likes, owned
    )
    new_lengths = new_lengths.reshape(rows * BLK)[:count]
    return (
        loglik.reshape(branches, 1, sites_here),
        parts.reshape(2, branches, owned),
        new_lengths,
    )


def solution(mesh):
    return jax.shard_map(
        compute,
        mesh=mesh,
        in_specs=(
            P(None, None, "dom", "site"),
            P(None, None, "dom", "site"),
            P("dom", None, None),
            P("dom", None, None),
            P("dom", None),
            P("dom", None),
            P("dom"),
            P(),
            P("dom", "site"),
            P("dom", "site"),
            P(),
        ),
        out_specs=(P(None, "dom", "site"), P(None, None, "dom"), P()),
        check_vma=False,
    )
```

```python
import functools

import jax
import jax.numpy as jnp
from jax import lax
from jax.experimental import pallas as pl
from jax.experimental.pallas import tpu as pltpu
from jax.sharding import PartitionSpec as P


BLK = 128
HALF = 64
SUB = 8
EARLY = 6
LOG2_E = 1.4426950408889634
F32 = jnp.float32
BF16 = jnp.bfloat16
LIMITS = pltpu.CompilerParams(vmem_limit_bytes=24 * 1024 * 1024)


def in_hbm(x):
    return pltpu.with_memory_space_constraint(x, pltpu.HBM)


def pack_kernel(
    rate_hbm,
    left_hbm,
    right_hbm,
    decay_hbm,
    weight_hbm,
    out_ref,
    right_ref,
    rate_ref,
    left_ref,
    decay_ref,
    weight_ref,
    small_sems,
    sems,
    right_sem,
):
    chunks, states, group, _ = left_ref.shape
    half = out_ref.shape[0]
    small = [
        pltpu.make_async_copy(src, dst, small_sems.at[i])
        for i, (src, dst) in enumerate(
            ((rate_hbm, rate_ref), (decay_hbm, decay_ref), (weight_hbm, weight_ref))
        )
    ]
    for copy in small:
        copy.start()

    def chunk_copy(g):
        rows = pl.ds(g * group, group)
        return pltpu.make_async_copy(left_hbm.at[:, rows, :], left_ref.at[g], sems.at[g])

    for g in range(chunks // 2):
        chunk_copy(g).start()
        chunk_copy(g + chunks // 2).start()
    right_copy = pltpu.make_async_copy(right_hbm, right_ref, right_sem)
    right_copy.start()
    for copy in small:
        copy.wait()
    left = left_ref.reshape(chunks * states * group, states)
    gap = jnp.zeros((states, HALF - states), F32)

    def beside(first, second):
        space = gap[: first.shape[0]]
        return jnp.concatenate([first, space, second, space], axis=1)

    def exponents(q):
        return -(decay_ref[pl.ds(q, 1), :] * rate_ref[q])

    for g in range(chunks // 2):
        chunk_copy(g).wait()
        chunk_copy(g + chunks // 2).wait()
        for i in range(group):
            q = g * group + i
            tables = [
                left[pl.ds(c * states * group + i, states, stride=group), :]
                for c in (g, g + chunks // 2)
            ]
            out_ref[q, pl.ds(0, states), :] = beside(*tables)
            out_ref[q, pl.ds(states, 1), :] = beside(exponents(q), exponents(q + half))
            out_ref[q, pl.ds(states + 1, 1), :] = beside(
                weight_ref[pl.ds(q, 1), :], weight_ref[pl.ds(q + half, 1), :]
            )
            rest = HALF - states - 2
            out_ref[q, pl.ds(states + 2, rest), :] = jnp.zeros((rest, 2 * HALF), F32)
    right_copy.wait()


def pack_tables(left, right, decay, weight, rate):
    states, parts, _ = left.shape
    group = 8
    chunks = parts // group
    hbm = pl.BlockSpec(memory_space=pltpu.HBM)
    row = pltpu.VMEM((parts, states), F32)
    return pl.pallas_call(
        pack_kernel,
        in_specs=[hbm] * 5,
        out_specs=[pl.BlockSpec(memory_space=pltpu.VMEM)] * 2,
        out_shape=[
            jax.ShapeDtypeStruct((parts // 2, HALF, 2 * HALF), F32),
            jax.ShapeDtypeStruct(right.shape, F32),
        ],
        scratch_shapes=[
            pltpu.SMEM((parts,), F32),
            pltpu.VMEM((chunks, states, group, states), F32),
            row,
            row,
            pltpu.SemaphoreType.DMA((3,)),
            pltpu.SemaphoreType.DMA((chunks,)),
            pltpu.SemaphoreType.DMA,
        ],
        name="pack",
        compiler_params=LIMITS,
    )(in_hbm(rate), in_hbm(left), in_hbm(right), in_hbm(decay), in_hbm(weight))


def copy_tiles(wanted_ref, own_left, own_right, partner_left, partner_right, *refs):
    out_refs, right_ref = refs[:-1], refs[-1]
    states, owned, _ = own_right.shape
    half = own_left.shape[0]
    base = lax.axis_index("dom") * owned
    rights = [ref.reshape(states * owned, states) for ref in (own_right, partner_right)]
    lane = lax.broadcasted_iota(jnp.int32, (HALF, 2 * HALF), 1)
    is_left = lane < HALF
    gap = jnp.zeros((states, 2 * HALF - states), F32)
    below = jnp.zeros((HALF - states, 2 * HALF), F32)
    for n in range(right_ref.shape[0]):
        part = wanted_ref[n]
        row = lax.rem(part, owned)
        mine = part - row == base

        @pl.when(mine)
        def _():
            right_ref[n] = rights[0][pl.ds(row, states, stride=owned), :]

        @pl.when(jnp.logical_not(mine))
        def _():
            right_ref[n] = rights[1][pl.ds(row, states, stride=owned), :]

    place = 0
    for out_ref in out_refs:
        for n in range(out_ref.shape[0]):
            part = wanted_ref[place]
            row = lax.rem(part, owned)
            mine = part - row == base

            def chosen(flag):
                return jnp.full((1, 2 * HALF), flag.astype(jnp.int32)) == 1

            second = row >= half
            at = jnp.where(second, row - half, row)
            left = jnp.where(chosen(mine), own_left[at], partner_left[at])
            left = jnp.where(chosen(second), pltpu.roll(left, HALF, 1), left)
            right = right_ref[place]
            right = jnp.concatenate([jnp.concatenate([right, gap], axis=1), below], axis=0)
            out_ref[n] = jnp.where(is_left, left, pltpu.roll(right, HALF, 1))
            place += 1


def pick_tiles(wanted, tables, pieces):
    vmem = pl.BlockSpec(memory_space=pltpu.VMEM)
    count = wanted.shape[0] // pieces
    return pl.pallas_call(
        copy_tiles,
        in_specs=[pl.BlockSpec(memory_space=pltpu.SMEM)] + [vmem] * 4,
        out_specs=[vmem] * pieces,
        out_shape=[jax.ShapeDtypeStruct((count, HALF, 2 * HALF), F32)] * pieces,
        scratch_shapes=[pltpu.VMEM(wanted.shape + tables[1].shape[::2], F32)],
        name="pick",
        compiler_params=LIMITS,
    )(wanted, *tables)


def start_split(skip, top_hbm, bottom_hbm, top_ref, bottom_ref, sems):
    chunks = sems.shape[1]
    chunk = top_ref.shape[0] // chunks

    def copies(g):
        there = pl.ds(g * chunk, chunk)
        here = pl.ds((skip + g) * chunk, chunk)
        return [
            pltpu.make_async_copy(src.at[here], dst.at[there], sems.at[i, g])
            for i, (src, dst) in enumerate(((top_hbm, top_ref), (bottom_hbm, bottom_ref)))
        ]

    for g in range(chunks):
        for copy in copies(g):
            copy.start()
    return copies


def finish_split(copies, out_ref, top_ref, bottom_ref, sems):
    nblocks = out_ref.shape[0]
    chunks = sems.shape[1]
    chunk = top_ref.shape[0] // chunks
    columns = out_ref.shape[3] // chunks
    fused = columns // BLK
    states = chunk // (fused * nblocks)
    pad = jnp.zeros((HALF - states, BLK), F32)

    def step(g, carry):
        for copy in copies(g):
            copy.wait()
        for b in range(fused):
            for n in range(nblocks):
                for side, ref in enumerate((top_ref, bottom_ref)):
                    first = g * chunk + b * states * nblocks + n
                    rows = ref[pl.ds(first, states, stride=nblocks), :]
                    full = jnp.concatenate([rows, pad], axis=0)
                    high = full.astype(BF16)
                    low = (full - high.astype(F32)).astype(BF16)
                    lanes = pl.ds(pl.multiple_of(g * columns + b * BLK, BLK), BLK)
                    out_ref[n, side, pl.ds(0, HALF), lanes] = high
                    out_ref[n, side, pl.ds(HALF, HALF), lanes] = low
        return carry

    lax.fori_loop(0, chunks, step, 0)


def early_kernel(top_hbm, bottom_hbm, out_ref, top_ref, bottom_ref, sems):
    copies = start_split(0, top_hbm, bottom_hbm, top_ref, bottom_ref, sems)
    finish_split(copies, out_ref, top_ref, bottom_ref, sems)


def late_kernel(
    skip,
    pair,
    rounds,
    blocks_hbm,
    chosen_hbm,
    lengths_hbm,
    padded_ref,
    top_hbm,
    bottom_hbm,
    own_left,
    own_right,
    partner_left,
    partner_right,
    out_ref,
    tiles_ref,
    aux_ref,
    map_ref,
    rows_ref,
    top_ref,
    bottom_ref,
    sems,
    right_ref,
    blocks_ref,
    chosen_ref,
    lengths_ref,
    small_sems,
):
    nblocks = out_ref.shape[0]
    branches = chosen_ref.shape[0]
    owned = own_right.shape[1]
    small = [
        pltpu.make_async_copy(src, dst, small_sems.at[i])
        for i, (src, dst) in enumerate(
            (
                (blocks_hbm, blocks_ref),
                (chosen_hbm, chosen_ref),
                (lengths_hbm, lengths_ref),
            )
        )
    ]
    for copy in small:
        copy.start()
    copies = start_split(skip, top_hbm, bottom_hbm, top_ref, bottom_ref, sems)
    for copy in small:
        copy.wait()
    copy_tiles(blocks_ref, own_left, own_right, partner_left, partner_right, tiles_ref, right_ref)
    my_pair = lax.axis_index("dom") // pair
    lane = lax.broadcasted_iota(jnp.int32, (1, BLK), 1)
    flat = lax.broadcasted_iota(jnp.int32, map_ref.shape, 0) * BLK
    flat = flat + lax.broadcasted_iota(jnp.int32, map_ref.shape, 1)
    for n in range(nblocks):
        part = blocks_ref[n]
        distance = lax.rem(lax.div(part, owned * pair) - my_pair + rounds, rounds)
        aux_ref[pl.ds(n, 1), :] = jnp.full((1, BLK), distance.astype(F32), F32)
        aux_ref[pl.ds(nblocks + n, 1), :] = jnp.full((1, BLK), part.astype(F32), F32)
    along = jnp.zeros((1, BLK), F32)
    update = jnp.zeros(map_ref.shape, jnp.int32)
    for b in range(branches):
        place = chosen_ref[b]
        time = lengths_ref[place]
        aux_ref[pl.ds(2 * nblocks + 8 + b, 1), :] = jnp.full((1, BLK), time, F32)
        along = jnp.where(lane == b, time, along)
        update = jnp.where(flat == place, b + 1, update)
    aux_ref[pl.ds(2 * nblocks, 1), :] = along
    map_ref[...] = update
    rows_ref[...] = padded_ref[...]
    finish_split(copies, out_ref, top_ref, bottom_ref, sems)


def split_scratch(top, branches, taken, fused):
    rows = top.shape[0] // branches * taken
    return [
        pltpu.VMEM((rows, BLK), F32),
        pltpu.VMEM((rows, BLK), F32),
        pltpu.SemaphoreType.DMA((2, taken // fused)),
    ]


def prepare_early(top, bottom, nblocks, branches, taken):
    hbm = pl.BlockSpec(memory_space=pltpu.HBM)
    return pl.pallas_call(
        early_kernel,
        in_specs=[hbm, hbm],
        out_specs=pl.BlockSpec(memory_space=pltpu.VMEM),
        out_shape=jax.ShapeDtypeStruct((nblocks, 2, 2 * HALF, taken * BLK), BF16),
        scratch_shapes=split_scratch(top, branches, taken, 2),
        name="early",
        compiler_params=LIMITS,
    )(in_hbm(top), in_hbm(bottom))


def prepare_late(
    blocks, chosen, lengths, padded, top, bottom, tables, skipped, pair, rounds
):
    nblocks = blocks.shape[0]
    branches = chosen.shape[0]
    taken = branches - skipped
    hbm = pl.BlockSpec(memory_space=pltpu.HBM)
    vmem = pl.BlockSpec(memory_space=pltpu.VMEM)
    return pl.pallas_call(
        functools.partial(late_kernel, skipped // 2, pair, rounds),
        in_specs=[hbm, hbm, hbm, vmem, hbm, hbm] + [vmem] * 4,
        out_specs=[vmem] * 5,
        out_shape=[
            jax.ShapeDtypeStruct((nblocks, 2, 2 * HALF, taken * BLK), BF16),
            jax.ShapeDtypeStruct((nblocks, HALF, 2 * HALF), F32),
            jax.ShapeDtypeStruct((2 * nblocks + 8 + branches, BLK), F32),
            jax.ShapeDtypeStruct(padded.shape, jnp.int32),
            jax.ShapeDtypeStruct(padded.shape, F32),
        ],
        scratch_shapes=split_scratch(top, branches, taken, 2)
        + [
            pltpu.VMEM((nblocks,) + tables[1].shape[::2], F32),
            pltpu.SMEM(blocks.shape, jnp.int32),
            pltpu.SMEM(chosen.shape, jnp.int32),
            pltpu.SMEM(lengths.shape, F32),
            pltpu.SemaphoreType.DMA((3,)),
        ],
        name="late",
        compiler_params=LIMITS,
    )(
        in_hbm(blocks),
        in_hbm(chosen),
        in_hbm(lengths),
        padded,
        in_hbm(top),
        in_hbm(bottom),
        *tables,
    )


def block_kernel(rounds, states, pieces, piece, aux_ref, weight_ref, early_ref, late_ref, own_ref, *refs):
    tiles = refs[: rounds - 1]
    earlier = refs[rounds - 1 : rounds - 1 + (piece if piece == pieces - 1 else 0)]
    like_ref, terms_ref, partial_ref = refs[-3:]
    branches, count, _ = like_ref.shape
    nblocks = early_ref.shape[0]
    split = early_ref.shape[3]
    start = piece * count
    wide = 2 * BLK
    lane = lax.broadcasted_iota(jnp.int32, (HALF, 2 * HALF), 1)
    is_left = lane < HALF
    for m in range(count):
        n = start + m
        distance = aux_ref[pl.ds(n, 1), :]
        tile = own_ref[n]
        for r in range(1, rounds):
            tile = jnp.where(distance == float(r), tiles[r - 1][m], tile)
        turned = pltpu.roll(tile, HALF, 1)
        flipped = tile[:, :HALF].T
        scaled = flipped * tile[states + 1 : states + 2, :HALF]
        left = jnp.concatenate([scaled, scaled], axis=1)
        sides = []
        for double in (left, jnp.where(is_left, turned, tile)):
            high = double.astype(BF16)
            low = (double - high.astype(F32)).astype(BF16)
            sides.append(jnp.concatenate([high, low[:, :HALF]], axis=1))
        expo = jnp.broadcast_to(flipped[:, states : states + 1], (HALF, BLK))
        powers = expo * LOG2_E
        for c in range(branches * BLK // wide):
            prods = []
            for side, lhs in enumerate(sides):
                if c * wide < split:
                    part = early_ref[n, side, :, pl.ds(c * wide, wide)]
                else:
                    part = late_ref[n, side, :, pl.ds(c * wide - split, wide)]
                rhs = jnp.concatenate([part, part[:HALF]], axis=0)
                prods.append(jnp.dot(lhs, rhs, preferred_element_type=F32))
            joint = prods[0] * prods[1]
            for h in range(wide // BLK):
                b = c * (wide // BLK) + h
                time = aux_ref[pl.ds(2 * nblocks + 8 + b, 1), :]
                zeroth = joint[:, h * BLK : (h + 1) * BLK] * jnp.exp2(powers * time)
                first = zeroth * expo
                second = first * expo
                for i, term in enumerate((zeroth, first, second)):
                    total = term[:SUB]
                    for k in range(SUB, HALF, SUB):
                        total = total + term[k : k + SUB]
                    partial_ref[i, b, pl.ds(m * SUB, SUB), :] = total

    weight = weight_ref[pl.ds(start, count), :].astype(F32)
    lanes = lax.broadcasted_iota(jnp.int32, (count, BLK), 1)
    terms = jnp.where(lanes == 2 * branches, aux_ref[pl.ds(nblocks + start, count), :], 0.0)
    for b in range(branches):
        sums = []
        for i in range(3):
            total = partial_ref[i, b, pl.ds(0, count, stride=SUB), :]
            for j in range(1, SUB):
                total = total + partial_ref[i, b, pl.ds(j, count, stride=SUB), :]
            sums.append(total)
        like_ref[b] = sums[0]
        inverse = 1.0 / sums[0]
        first = sums[1] * inverse
        second = sums[2] * inverse - first * first
        one = jnp.sum(weight * first, axis=1, keepdims=True)
        two = jnp.sum(weight * second, axis=1, keepdims=True)
        terms = jnp.where(lanes == b, one, terms)
        terms = jnp.where(lanes == branches + b, two, terms)
    if piece < pieces - 1:
        terms_ref[...] = terms
    else:
        terms = [ref[...] for ref in earlier] + [terms]
        for d in range(terms_ref.shape[0]):
            for i in range(0, pieces, 2):
                pair = terms[i] + pltpu.roll(terms[i + 1], HALF, 1)
                terms_ref[d, pl.ds(i // 2 * count, count), :] = pair


def block_likelihoods(
    aux, weight, operands, own_tiles, tiles, earlier, branches, states, devices, pieces, piece
):
    nblocks = operands[0].shape[0]
    count = nblocks // pieces
    vmem = pl.BlockSpec(memory_space=pltpu.VMEM)
    last = piece == pieces - 1
    return pl.pallas_call(
        functools.partial(block_kernel, len(tiles) + 1, states, pieces, piece),
        in_specs=[vmem] * (5 + len(tiles) + len(earlier)),
        out_specs=[vmem] * 2,
        out_shape=[
            jax.ShapeDtypeStruct((branches, count, BLK), F32),
            jax.ShapeDtypeStruct((devices, nblocks // 2, BLK) if last else (count, BLK), F32),
        ],
        scratch_shapes=[pltpu.VMEM((3, branches, count * SUB, BLK), F32)],
        name="blocks",
        compiler_params=LIMITS,
    )(aux, weight, *operands, own_tiles, *tiles, *earlier)


def sum_kernel(aux_ref, map_ref, lengths_ref, weight_ref, share_ref, *refs):
    like_refs = refs[:-3]
    part_ref, new_ref, loglik_ref = refs[-3:]
    branches, count, _ = like_refs[0].shape
    nblocks = count * len(like_refs)
    owned = part_ref.shape[1]
    terms = part_ref.shape[0]
    share = share_ref[...]
    share = jnp.concatenate([share, pltpu.roll(share, HALF, 1)], axis=0)
    share = share[:, :HALF]
    parts = lax.broadcasted_iota(jnp.int32, (share.shape[0], owned), 1)
    parts = parts + lax.axis_index("dom") * owned
    ident = share[:, terms : terms + 1].astype(jnp.int32)
    onehot = (ident == parts).astype(F32)
    sums = lax.dot_general(
        share,
        onehot,
        (((0,), (0,)), ((), ())),
        precision=lax.Precision.HIGHEST,
        preferred_element_type=F32,
    )
    part_ref[...] = sums[:terms]
    total = jnp.sum(share, axis=0, keepdims=True)
    total = jnp.concatenate([total, total], axis=1)
    second = pltpu.roll(total, BLK - branches, 1)
    updated = aux_ref[pl.ds(2 * nblocks, 1), :] - total / second
    lane = lax.broadcasted_iota(jnp.int32, (1, BLK), 1)
    place = map_ref[...]
    new = lengths_ref[...]
    for b in range(branches):
        value = jnp.sum(jnp.where(lane == b, updated, 0.0), axis=1, keepdims=True)
        new = jnp.where(place == b + 1, value, new)
    new_ref[...] = new
    for i, like_ref in enumerate(like_refs):
        blocks = pl.ds(i * count, count)
        weight = weight_ref[blocks, :].astype(F32)
        for b in range(branches):
            loglik_ref[b, blocks, :] = weight * jnp.log(like_ref[b])


def add_up(aux, places, lengths, weight, share, likes, owned):
    vmem = pl.BlockSpec(memory_space=pltpu.VMEM)
    branches = likes[0].shape[0]
    nblocks = weight.shape[0]
    return pl.pallas_call(
        sum_kernel,
        in_specs=[vmem] * (5 + len(likes)),
        out_specs=[vmem] * 3,
        out_shape=[
            jax.ShapeDtypeStruct((2 * branches, owned), F32),
            jax.ShapeDtypeStruct(lengths.shape, F32),
            jax.ShapeDtypeStruct((branches, nblocks, BLK), F32),
        ],
        name="sums",
        compiler_params=LIMITS,
    )(aux, places, lengths, weight, share, *likes)


def compute(
    top_partial,
    bottom_partial,
    left_vectors,
    right_vectors,
    decay_rates,
    state_weights,
    part_rates,
    branch_lengths,
    pattern_weights,
    block_partition,
    chosen_branches,
):
    branches, states, _, sites_here = top_partial.shape
    nblocks = sites_here // BLK
    owned = left_vectors.shape[0]
    groups = lax.axis_size("dom")
    pair = 2 if groups % 2 == 0 else 1
    rounds = groups // pair

    def shifted(value, r):
        step = [
            (d, ((d // pair + r) % rounds) * pair + d % pair) for d in range(groups)
        ]
        return lax.ppermute(value, "dom", step)

    blocks = block_partition[0]
    requests = [shifted(blocks, rounds - r) for r in range(1, rounds)]
    left_turned = jnp.transpose(left_vectors, (1, 0, 2))
    right_turned = jnp.transpose(right_vectors, (1, 0, 2))

    def swapped(value):
        if pair == 1:
            return value
        return lax.ppermute(value, "dom", [(d, d ^ 1) for d in range(groups)])

    partner_right = swapped(right_turned)
    own = pack_tables(left_turned, right_turned, decay_rates, state_weights, part_rates)
    partner_left = swapped(own[0])
    tables = [*own, partner_left, partner_right]
    pieces = 2
    answers = []
    for r, request in zip(range(1, rounds), requests):
        answers.append([shifted(t, r) for t in pick_tiles(request, tables, pieces)])
    count = branch_lengths.shape[0]
    rows = -(-count // BLK)
    padded = jnp.pad(branch_lengths, (0, rows * BLK - count)).reshape(rows, BLK)
    top = top_partial.reshape(branches * states * nblocks, BLK)
    bottom = bottom_partial.reshape(branches * states * nblocks, BLK)
    early = prepare_early(top, bottom, nblocks, branches, EARLY)
    late, tiles, aux, places, lengths = prepare_late(
        blocks,
        chosen_branches,
        branch_lengths,
        padded,
        top,
        bottom,
        tables,
        EARLY,
        pair,
        rounds,
    )
    operands = [early, late]
    answers = answers[::-1]
    devices = lax.axis_size("site") * groups
    weight = pattern_weights.reshape(nblocks, BLK)
    likes, earlier = [], []
    for piece in range(pieces):
        like, terms = block_likelihoods(
            aux,
            weight,
            operands,
            tiles,
            [answer[piece] for answer in answers],
            earlier,
            branches,
            states,
            devices,
            pieces,
            piece,
        )
        likes.append(like)
        earlier.append(terms)
    everything = lax.all_to_all(
        terms, ("site", "dom"), split_axis=0, concat_axis=0, tiled=True
    )
    parts, new_lengths, loglik = add_up(
        aux, places, lengths, weight, everything.reshape(-1, BLK), likes, owned
    )
    new_lengths = new_lengths.reshape(rows * BLK)[:count]
    return (
        loglik.reshape(branches, 1, sites_here),
        parts.reshape(2, branches, owned),
        new_lengths,
    )


def solution(mesh):
    return jax.shard_map(
        compute,
        mesh=mesh,
        in_specs=(
            P(None, None, "dom", "site"),
            P(None, None, "dom", "site"),
            P("dom", None, None),
            P("dom", None, None),
            P("dom", None),
            P("dom", None),
            P("dom"),
            P(),
            P("dom", "site"),
            P("dom", "site"),
            P(),
        ),
        out_specs=(P(None, "dom", "site"), P(None, None, "dom"), P()),
        check_vma=False,
    )
```

```python
import functools

import jax
import jax.numpy as jnp
from jax import lax
from jax.experimental import pallas as pl
from jax.experimental.pallas import tpu as pltpu
from jax.sharding import PartitionSpec as P


BLK = 128
HALF = 64
SUB = 8
EARLY = 6
LOG2_E = 1.4426950408889634
F32 = jnp.float32
BF16 = jnp.bfloat16
LIMITS = pltpu.CompilerParams(vmem_limit_bytes=24 * 1024 * 1024)


def in_hbm(x):
    return pltpu.with_memory_space_constraint(x, pltpu.HBM)


def pack_kernel(
    rate_hbm,
    left_hbm,
    right_hbm,
    decay_hbm,
    weight_hbm,
    out_ref,
    right_ref,
    rate_ref,
    left_ref,
    decay_ref,
    weight_ref,
    small_sems,
    sems,
    right_sem,
):
    chunks, states, group, _ = left_ref.shape
    half = out_ref.shape[0]
    small = [
        pltpu.make_async_copy(src, dst, small_sems.at[i])
        for i, (src, dst) in enumerate(
            ((rate_hbm, rate_ref), (decay_hbm, decay_ref), (weight_hbm, weight_ref))
        )
    ]
    for copy in small:
        copy.start()

    def chunk_copy(g):
        rows = pl.ds(g * group, group)
        return pltpu.make_async_copy(left_hbm.at[:, rows, :], left_ref.at[g], sems.at[g])

    for g in range(chunks // 2):
        chunk_copy(g).start()
        chunk_copy(g + chunks // 2).start()
    right_copy = pltpu.make_async_copy(right_hbm, right_ref, right_sem)
    right_copy.start()
    for copy in small:
        copy.wait()
    left = left_ref.reshape(chunks * states * group, states)
    gap = jnp.zeros((states, HALF - states), F32)

    def beside(first, second):
        space = gap[: first.shape[0]]
        return jnp.concatenate([first, space, second, space], axis=1)

    def exponents(q):
        return -(decay_ref[pl.ds(q, 1), :] * rate_ref[q])

    for g in range(chunks // 2):
        chunk_copy(g).wait()
        chunk_copy(g + chunks // 2).wait()
        for i in range(group):
            q = g * group + i
            tables = [
                left[pl.ds(c * states * group + i, states, stride=group), :]
                for c in (g, g + chunks // 2)
            ]
            out_ref[q, pl.ds(0, states), :] = beside(*tables)
            out_ref[q, pl.ds(states, 1), :] = beside(exponents(q), exponents(q + half))
            out_ref[q, pl.ds(states + 1, 1), :] = beside(
                weight_ref[pl.ds(q, 1), :], weight_ref[pl.ds(q + half, 1), :]
            )
            rest = HALF - states - 2
            out_ref[q, pl.ds(states + 2, rest), :] = jnp.zeros((rest, 2 * HALF), F32)
    right_copy.wait()


def pack_tables(left, right, decay, weight, rate):
    states, parts, _ = left.shape
    group = 8
    chunks = parts // group
    hbm = pl.BlockSpec(memory_space=pltpu.HBM)
    row = pltpu.VMEM((parts, states), F32)
    return pl.pallas_call(
        pack_kernel,
        in_specs=[hbm] * 5,
        out_specs=[pl.BlockSpec(memory_space=pltpu.VMEM)] * 2,
        out_shape=[
            jax.ShapeDtypeStruct((parts // 2, HALF, 2 * HALF), F32),
            jax.ShapeDtypeStruct(right.shape, F32),
        ],
        scratch_shapes=[
            pltpu.SMEM((parts,), F32),
            pltpu.VMEM((chunks, states, group, states), F32),
            row,
            row,
            pltpu.SemaphoreType.DMA((3,)),
            pltpu.SemaphoreType.DMA((chunks,)),
            pltpu.SemaphoreType.DMA,
        ],
        name="pack",
        compiler_params=LIMITS,
    )(in_hbm(rate), in_hbm(left), in_hbm(right), in_hbm(decay), in_hbm(weight))


def copy_tiles(wanted_ref, own_left, own_right, partner_left, partner_right, *refs):
    out_refs, right_ref = refs[:-1], refs[-1]
    states, owned, _ = own_right.shape
    half = own_left.shape[0]
    base = lax.axis_index("dom") * owned
    rights = [ref.reshape(states * owned, states) for ref in (own_right, partner_right)]
    lane = lax.broadcasted_iota(jnp.int32, (HALF, 2 * HALF), 1)
    is_left = lane < HALF
    gap = jnp.zeros((states, 2 * HALF - states), F32)
    below = jnp.zeros((HALF - states - 1, 2 * HALF), F32)
    for n in range(right_ref.shape[0]):
        part = wanted_ref[n]
        row = lax.rem(part, owned)
        mine = part - row == base

        @pl.when(mine)
        def _():
            right_ref[n] = rights[0][pl.ds(row, states, stride=owned), :]

        @pl.when(jnp.logical_not(mine))
        def _():
            right_ref[n] = rights[1][pl.ds(row, states, stride=owned), :]

    place = 0
    for out_ref in out_refs:
        tall = HALF if len(out_ref.shape) == 3 else states + 1
        for n in range(out_ref.size // (tall * 2 * HALF)):
            part = wanted_ref[place]
            row = lax.rem(part, owned)
            mine = part - row == base

            def chosen(flag):
                return jnp.full((1, 2 * HALF), flag.astype(jnp.int32)) == 1

            second = row >= half
            at = jnp.where(second, row - half, row)
            left = jnp.where(chosen(mine), own_left[at], partner_left[at])
            left = jnp.where(chosen(second), pltpu.roll(left, HALF, 1), left)
            right = right_ref[place]
            right = jnp.concatenate(
                [jnp.concatenate([right, gap], axis=1), left[states + 1 : states + 2], below],
                axis=0,
            )
            tile = jnp.where(is_left, left, pltpu.roll(right, HALF, 1))
            if len(out_ref.shape) == 3:
                out_ref[n] = tile
            else:
                out_ref[pl.ds(n * (states + 1), states + 1), :] = tile[: states + 1]
            place += 1


def pick_tiles(wanted, tables, pieces):
    vmem = pl.BlockSpec(memory_space=pltpu.VMEM)
    count = wanted.shape[0] // pieces
    rows = tables[1].shape[0] + 1
    return pl.pallas_call(
        copy_tiles,
        in_specs=[pl.BlockSpec(memory_space=pltpu.SMEM)] + [vmem] * 4,
        out_specs=[vmem] * pieces,
        out_shape=[jax.ShapeDtypeStruct((count * rows, 2 * HALF), F32)] * pieces,
        scratch_shapes=[pltpu.VMEM(wanted.shape + tables[1].shape[::2], F32)],
        name="pick",
        compiler_params=LIMITS,
    )(wanted, *tables)


def start_split(skip, top_hbm, bottom_hbm, top_ref, bottom_ref, sems):
    chunks = sems.shape[1]
    chunk = top_ref.shape[0] // chunks

    def copies(g):
        there = pl.ds(g * chunk, chunk)
        here = pl.ds((skip + g) * chunk, chunk)
        return [
            pltpu.make_async_copy(src.at[here], dst.at[there], sems.at[i, g])
            for i, (src, dst) in enumerate(((top_hbm, top_ref), (bottom_hbm, bottom_ref)))
        ]

    for g in range(chunks):
        for copy in copies(g):
            copy.start()
    return copies


def finish_split(copies, out_ref, top_ref, bottom_ref, sems):
    nblocks = out_ref.shape[0]
    chunks = sems.shape[1]
    chunk = top_ref.shape[0] // chunks
    columns = out_ref.shape[3] // chunks
    fused = columns // BLK
    states = chunk // (fused * nblocks)
    pad = jnp.zeros((HALF - states, BLK), F32)

    def step(g, carry):
        for copy in copies(g):
            copy.wait()
        for b in range(fused):
            for n in range(nblocks):
                for side, ref in enumerate((top_ref, bottom_ref)):
                    first = g * chunk + b * states * nblocks + n
                    rows = ref[pl.ds(first, states, stride=nblocks), :]
                    full = jnp.concatenate([rows, pad], axis=0)
                    high = full.astype(BF16)
                    low = (full - high.astype(F32)).astype(BF16)
                    lanes = pl.ds(pl.multiple_of(g * columns + b * BLK, BLK), BLK)
                    out_ref[n, side, pl.ds(0, HALF), lanes] = high
                    out_ref[n, side, pl.ds(HALF, HALF), lanes] = low
        return carry

    lax.fori_loop(0, chunks, step, 0)


def early_kernel(top_hbm, bottom_hbm, out_ref, top_ref, bottom_ref, sems):
    copies = start_split(0, top_hbm, bottom_hbm, top_ref, bottom_ref, sems)
    finish_split(copies, out_ref, top_ref, bottom_ref, sems)


def late_kernel(
    skip,
    pair,
    rounds,
    blocks_hbm,
    chosen_hbm,
    lengths_hbm,
    padded_ref,
    top_hbm,
    bottom_hbm,
    own_left,
    own_right,
    partner_left,
    partner_right,
    out_ref,
    tiles_ref,
    aux_ref,
    map_ref,
    rows_ref,
    top_ref,
    bottom_ref,
    sems,
    right_ref,
    blocks_ref,
    chosen_ref,
    lengths_ref,
    small_sems,
):
    nblocks = out_ref.shape[0]
    branches = chosen_ref.shape[0]
    owned = own_right.shape[1]
    small = [
        pltpu.make_async_copy(src, dst, small_sems.at[i])
        for i, (src, dst) in enumerate(
            (
                (blocks_hbm, blocks_ref),
                (chosen_hbm, chosen_ref),
                (lengths_hbm, lengths_ref),
            )
        )
    ]
    for copy in small:
        copy.start()
    copies = start_split(skip, top_hbm, bottom_hbm, top_ref, bottom_ref, sems)
    for copy in small:
        copy.wait()
    copy_tiles(blocks_ref, own_left, own_right, partner_left, partner_right, tiles_ref, right_ref)
    my_pair = lax.axis_index("dom") // pair
    lane = lax.broadcasted_iota(jnp.int32, (1, BLK), 1)
    flat = lax.broadcasted_iota(jnp.int32, map_ref.shape, 0) * BLK
    flat = flat + lax.broadcasted_iota(jnp.int32, map_ref.shape, 1)
    for n in range(nblocks):
        part = blocks_ref[n]
        distance = lax.rem(lax.div(part, owned * pair) - my_pair + rounds, rounds)
        aux_ref[pl.ds(n, 1), :] = jnp.full((1, BLK), distance.astype(F32), F32)
        aux_ref[pl.ds(nblocks + n, 1), :] = jnp.full((1, BLK), part.astype(F32), F32)
    along = jnp.zeros((1, BLK), F32)
    update = jnp.zeros(map_ref.shape, jnp.int32)
    for b in range(branches):
        place = chosen_ref[b]
        time = lengths_ref[place]
        aux_ref[pl.ds(2 * nblocks + 8 + b, 1), :] = jnp.full((1, BLK), time, F32)
        along = jnp.where(lane == b, time, along)
        update = jnp.where(flat == place, b + 1, update)
    aux_ref[pl.ds(2 * nblocks, 1), :] = along
    map_ref[...] = update
    rows_ref[...] = padded_ref[...]
    finish_split(copies, out_ref, top_ref, bottom_ref, sems)


def split_scratch(top, branches, taken, fused):
    rows = top.shape[0] // branches * taken
    return [
        pltpu.VMEM((rows, BLK), F32),
        pltpu.VMEM((rows, BLK), F32),
        pltpu.SemaphoreType.DMA((2, taken // fused)),
    ]


def prepare_early(top, bottom, nblocks, branches, taken):
    hbm = pl.BlockSpec(memory_space=pltpu.HBM)
    return pl.pallas_call(
        early_kernel,
        in_specs=[hbm, hbm],
        out_specs=pl.BlockSpec(memory_space=pltpu.VMEM),
        out_shape=jax.ShapeDtypeStruct((nblocks, 2, 2 * HALF, taken * BLK), BF16),
        scratch_shapes=split_scratch(top, branches, taken, 2),
        name="early",
        compiler_params=LIMITS,
    )(in_hbm(top), in_hbm(bottom))


def prepare_late(
    blocks, chosen, lengths, padded, top, bottom, tables, skipped, pair, rounds
):
    nblocks = blocks.shape[0]
    branches = chosen.shape[0]
    taken = branches - skipped
    hbm = pl.BlockSpec(memory_space=pltpu.HBM)
    vmem = pl.BlockSpec(memory_space=pltpu.VMEM)
    return pl.pallas_call(
        functools.partial(late_kernel, skipped // 2, pair, rounds),
        in_specs=[hbm, hbm, hbm, vmem, hbm, hbm] + [vmem] * 4,
        out_specs=[vmem] * 5,
        out_shape=[
            jax.ShapeDtypeStruct((nblocks, 2, 2 * HALF, taken * BLK), BF16),
            jax.ShapeDtypeStruct((nblocks, HALF, 2 * HALF), F32),
            jax.ShapeDtypeStruct((2 * nblocks + 8 + branches, BLK), F32),
            jax.ShapeDtypeStruct(padded.shape, jnp.int32),
            jax.ShapeDtypeStruct(padded.shape, F32),
        ],
        scratch_shapes=split_scratch(top, branches, taken, 2)
        + [
            pltpu.VMEM((nblocks,) + tables[1].shape[::2], F32),
            pltpu.SMEM(blocks.shape, jnp.int32),
            pltpu.SMEM(chosen.shape, jnp.int32),
            pltpu.SMEM(lengths.shape, F32),
            pltpu.SemaphoreType.DMA((3,)),
        ],
        name="late",
        compiler_params=LIMITS,
    )(
        in_hbm(blocks),
        in_hbm(chosen),
        in_hbm(lengths),
        padded,
        in_hbm(top),
        in_hbm(bottom),
        *tables,
    )


def block_kernel(rounds, states, pieces, piece, aux_ref, weight_ref, early_ref, late_ref, own_ref, *refs):
    tiles = refs[: rounds - 1]
    earlier = refs[rounds - 1 : rounds - 1 + (piece if piece == pieces - 1 else 0)]
    like_ref, terms_ref, partial_ref = refs[-3:]
    branches, count, _ = like_ref.shape
    nblocks = early_ref.shape[0]
    split = early_ref.shape[3]
    start = piece * count
    wide = 2 * BLK
    lane = lax.broadcasted_iota(jnp.int32, (HALF, 2 * HALF), 1)
    is_left = lane < HALF
    for m in range(count):
        n = start + m
        distance = aux_ref[pl.ds(n, 1), :]
        tile = own_ref[n]
        for r in range(1, rounds):
            sent = tiles[r - 1][pl.ds(m * (states + 1), states + 1), :]
            sent = jnp.concatenate([sent, jnp.zeros((HALF - states - 1, 2 * HALF), F32)], axis=0)
            tile = jnp.where(distance == float(r), sent, tile)
        turned = pltpu.roll(tile, HALF, 1)
        flipped = tile[:, :HALF].T
        scaled = flipped * turned[states : states + 1, :HALF]
        left = jnp.concatenate([scaled, scaled], axis=1)
        sides = []
        for double in (left, jnp.where(is_left, turned, tile)):
            high = double.astype(BF16)
            low = (double - high.astype(F32)).astype(BF16)
            sides.append(jnp.concatenate([high, low[:, :HALF]], axis=1))
        expo = jnp.broadcast_to(flipped[:, states : states + 1], (HALF, BLK))
        powers = expo * LOG2_E
        for c in range(branches * BLK // wide):
            prods = []
            for side, lhs in enumerate(sides):
                if c * wide < split:
                    part = early_ref[n, side, :, pl.ds(c * wide, wide)]
                else:
                    part = late_ref[n, side, :, pl.ds(c * wide - split, wide)]
                rhs = jnp.concatenate([part, part[:HALF]], axis=0)
                prods.append(jnp.dot(lhs, rhs, preferred_element_type=F32))
            joint = prods[0] * prods[1]
            for h in range(wide // BLK):
                b = c * (wide // BLK) + h
                time = aux_ref[pl.ds(2 * nblocks + 8 + b, 1), :]
                zeroth = joint[:, h * BLK : (h + 1) * BLK] * jnp.exp2(powers * time)
                first = zeroth * expo
                second = first * expo
                for i, term in enumerate((zeroth, first, second)):
                    total = term[:SUB]
                    for k in range(SUB, HALF, SUB):
                        total = total + term[k : k + SUB]
                    partial_ref[i, b, pl.ds(m * SUB, SUB), :] = total

    weight = weight_ref[pl.ds(start, count), :].astype(F32)
    lanes = lax.broadcasted_iota(jnp.int32, (count, BLK), 1)
    terms = jnp.where(lanes == 2 * branches, aux_ref[pl.ds(nblocks + start, count), :], 0.0)
    for b in range(branches):
        sums = []
        for i in range(3):
            total = partial_ref[i, b, pl.ds(0, count, stride=SUB), :]
            for j in range(1, SUB):
                total = total + partial_ref[i, b, pl.ds(j, count, stride=SUB), :]
            sums.append(total)
        like_ref[b] = sums[0]
        inverse = 1.0 / sums[0]
        first = sums[1] * inverse
        second = sums[2] * inverse - first * first
        one = jnp.sum(weight * first, axis=1, keepdims=True)
        two = jnp.sum(weight * second, axis=1, keepdims=True)
        terms = jnp.where(lanes == b, one, terms)
        terms = jnp.where(lanes == branches + b, two, terms)
    if piece < pieces - 1:
        terms_ref[...] = terms
    else:
        terms = [ref[...] for ref in earlier] + [terms]
        for d in range(terms_ref.shape[0]):
            for i in range(0, pieces, 2):
                pair = terms[i] + pltpu.roll(terms[i + 1], HALF, 1)
                terms_ref[d, pl.ds(i // 2 * count, count), :] = pair


def block_likelihoods(
    aux, weight, operands, own_tiles, tiles, earlier, branches, states, devices, pieces, piece
):
    nblocks = operands[0].shape[0]
    count = nblocks // pieces
    vmem = pl.BlockSpec(memory_space=pltpu.VMEM)
    last = piece == pieces - 1
    return pl.pallas_call(
        functools.partial(block_kernel, len(tiles) + 1, states, pieces, piece),
        in_specs=[vmem] * (5 + len(tiles) + len(earlier)),
        out_specs=[vmem] * 2,
        out_shape=[
            jax.ShapeDtypeStruct((branches, count, BLK), F32),
            jax.ShapeDtypeStruct((devices, nblocks // 2, BLK) if last else (count, BLK), F32),
        ],
        scratch_shapes=[pltpu.VMEM((3, branches, count * SUB, BLK), F32)],
        name="blocks",
        compiler_params=LIMITS,
    )(aux, weight, *operands, own_tiles, *tiles, *earlier)


def sum_kernel(aux_ref, map_ref, lengths_ref, weight_ref, share_ref, *refs):
    like_refs = refs[:-3]
    part_ref, new_ref, loglik_ref = refs[-3:]
    branches, count, _ = like_refs[0].shape
    nblocks = count * len(like_refs)
    owned = part_ref.shape[1]
    terms = part_ref.shape[0]
    share = share_ref[...]
    share = jnp.concatenate([share, pltpu.roll(share, HALF, 1)], axis=0)
    share = share[:, :HALF]
    parts = lax.broadcasted_iota(jnp.int32, (share.shape[0], owned), 1)
    parts = parts + lax.axis_index("dom") * owned
    ident = share[:, terms : terms + 1].astype(jnp.int32)
    onehot = (ident == parts).astype(F32)
    sums = lax.dot_general(
        share,
        onehot,
        (((0,), (0,)), ((), ())),
        precision=lax.Precision.HIGHEST,
        preferred_element_type=F32,
    )
    part_ref[...] = sums[:terms]
    total = jnp.sum(share, axis=0, keepdims=True)
    total = jnp.concatenate([total, total], axis=1)
    second = pltpu.roll(total, BLK - branches, 1)
    updated = aux_ref[pl.ds(2 * nblocks, 1), :] - total / second
    lane = lax.broadcasted_iota(jnp.int32, (1, BLK), 1)
    place = map_ref[...]
    new = lengths_ref[...]
    for b in range(branches):
        value = jnp.sum(jnp.where(lane == b, updated, 0.0), axis=1, keepdims=True)
        new = jnp.where(place == b + 1, value, new)
    new_ref[...] = new
    for i, like_ref in enumerate(like_refs):
        blocks = pl.ds(i * count, count)
        weight = weight_ref[blocks, :].astype(F32)
        for b in range(branches):
            loglik_ref[b, blocks, :] = weight * jnp.log(like_ref[b])


def add_up(aux, places, lengths, weight, share, likes, owned):
    vmem = pl.BlockSpec(memory_space=pltpu.VMEM)
    branches = likes[0].shape[0]
    nblocks = weight.shape[0]
    return pl.pallas_call(
        sum_kernel,
        in_specs=[vmem] * (5 + len(likes)),
        out_specs=[vmem] * 3,
        out_shape=[
            jax.ShapeDtypeStruct((2 * branches, owned), F32),
            jax.ShapeDtypeStruct(lengths.shape, F32),
            jax.ShapeDtypeStruct((branches, nblocks, BLK), F32),
        ],
        name="sums",
        compiler_params=LIMITS,
    )(aux, places, lengths, weight, share, *likes)


def compute(
    top_partial,
    bottom_partial,
    left_vectors,
    right_vectors,
    decay_rates,
    state_weights,
    part_rates,
    branch_lengths,
    pattern_weights,
    block_partition,
    chosen_branches,
):
    branches, states, _, sites_here = top_partial.shape
    nblocks = sites_here // BLK
    owned = left_vectors.shape[0]
    groups = lax.axis_size("dom")
    pair = 2 if groups % 2 == 0 else 1
    rounds = groups // pair

    def shifted(value, r):
        step = [
            (d, ((d // pair + r) % rounds) * pair + d % pair) for d in range(groups)
        ]
        return lax.ppermute(value, "dom", step)

    blocks = block_partition[0]
    requests = [shifted(blocks, rounds - r) for r in range(1, rounds)]
    left_turned = jnp.transpose(left_vectors, (1, 0, 2))
    right_turned = jnp.transpose(right_vectors, (1, 0, 2))

    def swapped(value):
        if pair == 1:
            return value
        return lax.ppermute(value, "dom", [(d, d ^ 1) for d in range(groups)])

    partner_right = swapped(right_turned)
    own = pack_tables(left_turned, right_turned, decay_rates, state_weights, part_rates)
    partner_left = swapped(own[0])
    tables = [*own, partner_left, partner_right]
    pieces = 2
    answers = []
    for r, request in zip(range(1, rounds), requests):
        answers.append([shifted(t, r) for t in pick_tiles(request, tables, pieces)])
    count = branch_lengths.shape[0]
    rows = -(-count // BLK)
    padded = jnp.pad(branch_lengths, (0, rows * BLK - count)).reshape(rows, BLK)
    top = top_partial.reshape(branches * states * nblocks, BLK)
    bottom = bottom_partial.reshape(branches * states * nblocks, BLK)
    early = prepare_early(top, bottom, nblocks, branches, EARLY)
    late, tiles, aux, places, lengths = prepare_late(
        blocks,
        chosen_branches,
        branch_lengths,
        padded,
        top,
        bottom,
        tables,
        EARLY,
        pair,
        rounds,
    )
    operands = [early, late]
    answers = answers[::-1]
    devices = lax.axis_size("site") * groups
    weight = pattern_weights.reshape(nblocks, BLK)
    likes, earlier = [], []
    for piece in range(pieces):
        like, terms = block_likelihoods(
            aux,
            weight,
            operands,
            tiles,
            [answer[piece] for answer in answers],
            earlier,
            branches,
            states,
            devices,
            pieces,
            piece,
        )
        likes.append(like)
        earlier.append(terms)
    everything = lax.all_to_all(
        terms, ("site", "dom"), split_axis=0, concat_axis=0, tiled=True
    )
    parts, new_lengths, loglik = add_up(
        aux, places, lengths, weight, everything.reshape(-1, BLK), likes, owned
    )
    new_lengths = new_lengths.reshape(rows * BLK)[:count]
    return (
        loglik.reshape(branches, 1, sites_here),
        parts.reshape(2, branches, owned),
        new_lengths,
    )


def solution(mesh):
    return jax.shard_map(
        compute,
        mesh=mesh,
        in_specs=(
            P(None, None, "dom", "site"),
            P(None, None, "dom", "site"),
            P("dom", None, None),
            P("dom", None, None),
            P("dom", None),
            P("dom", None),
            P("dom"),
            P(),
            P("dom", "site"),
            P("dom", "site"),
            P(),
        ),
        out_specs=(P(None, "dom", "site"), P(None, None, "dom"), P()),
        check_vma=False,
    )
```

```python
import functools

import jax
import jax.numpy as jnp
from jax import lax
from jax.experimental import pallas as pl
from jax.experimental.pallas import tpu as pltpu
from jax.sharding import PartitionSpec as P


BLK = 128
HALF = 64
SUB = 8
EARLY = 2
LOG2_E = 1.4426950408889634
F32 = jnp.float32
BF16 = jnp.bfloat16
LIMITS = pltpu.CompilerParams(vmem_limit_bytes=24 * 1024 * 1024)


def in_hbm(x):
    return pltpu.with_memory_space_constraint(x, pltpu.HBM)


def pack_kernel(
    rate_hbm,
    left_hbm,
    right_hbm,
    decay_hbm,
    weight_hbm,
    out_ref,
    right_ref,
    rate_ref,
    left_ref,
    decay_ref,
    weight_ref,
    small_sems,
    sems,
    right_sem,
):
    chunks, states, group, _ = left_ref.shape
    half = out_ref.shape[0]
    small = [
        pltpu.make_async_copy(src, dst, small_sems.at[i])
        for i, (src, dst) in enumerate(
            ((rate_hbm, rate_ref), (decay_hbm, decay_ref), (weight_hbm, weight_ref))
        )
    ]
    for copy in small:
        copy.start()

    def chunk_copy(g):
        rows = pl.ds(g * group, group)
        return pltpu.make_async_copy(left_hbm.at[:, rows, :], left_ref.at[g], sems.at[g])

    for g in range(chunks // 2):
        chunk_copy(g).start()
        chunk_copy(g + chunks // 2).start()
    right_copy = pltpu.make_async_copy(right_hbm, right_ref, right_sem)
    right_copy.start()
    for copy in small:
        copy.wait()
    left = left_ref.reshape(chunks * states * group, states)
    gap = jnp.zeros((states, HALF - states), F32)

    def beside(first, second):
        space = gap[: first.shape[0]]
        return jnp.concatenate([first, space, second, space], axis=1)

    def exponents(q):
        return -(decay_ref[pl.ds(q, 1), :] * rate_ref[q])

    for g in range(chunks // 2):
        chunk_copy(g).wait()
        chunk_copy(g + chunks // 2).wait()
        for i in range(group):
            q = g * group + i
            tables = [
                left[pl.ds(c * states * group + i, states, stride=group), :]
                for c in (g, g + chunks // 2)
            ]
            out_ref[q, pl.ds(0, states), :] = beside(*tables)
            out_ref[q, pl.ds(states, 1), :] = beside(exponents(q), exponents(q + half))
            out_ref[q, pl.ds(states + 1, 1), :] = beside(
                weight_ref[pl.ds(q, 1), :], weight_ref[pl.ds(q + half, 1), :]
            )
            rest = HALF - states - 2
            out_ref[q, pl.ds(states + 2, rest), :] = jnp.zeros((rest, 2 * HALF), F32)
    right_copy.wait()


def pack_tables(left, right, decay, weight, rate):
    states, parts, _ = left.shape
    group = 8
    chunks = parts // group
    hbm = pl.BlockSpec(memory_space=pltpu.HBM)
    row = pltpu.VMEM((parts, states), F32)
    return pl.pallas_call(
        pack_kernel,
        in_specs=[hbm] * 5,
        out_specs=[pl.BlockSpec(memory_space=pltpu.VMEM)] * 2,
        out_shape=[
            jax.ShapeDtypeStruct((parts // 2, HALF, 2 * HALF), F32),
            jax.ShapeDtypeStruct(right.shape, F32),
        ],
        scratch_shapes=[
            pltpu.SMEM((parts,), F32),
            pltpu.VMEM((chunks, states, group, states), F32),
            row,
            row,
            pltpu.SemaphoreType.DMA((3,)),
            pltpu.SemaphoreType.DMA((chunks,)),
            pltpu.SemaphoreType.DMA,
        ],
        name="pack",
        compiler_params=LIMITS,
    )(in_hbm(rate), in_hbm(left), in_hbm(right), in_hbm(decay), in_hbm(weight))


def copy_tiles(wanted_ref, own_left, own_right, partner_left, partner_right, *refs):
    copy_rights(wanted_ref, own_right, partner_right, refs[-1])
    join_tiles(wanted_ref, own_left, partner_left, refs[-1], *refs[:-1])


def copy_rights(wanted_ref, own_right, partner_right, right_ref):
    states, owned, _ = own_right.shape
    base = lax.axis_index("dom") * owned
    rights = [ref.reshape(states * owned, states) for ref in (own_right, partner_right)]
    for n in range(right_ref.shape[0]):
        part = wanted_ref[n]
        row = lax.rem(part, owned)
        mine = part - row == base

        @pl.when(mine)
        def _():
            right_ref[n] = rights[0][pl.ds(row, states, stride=owned), :]

        @pl.when(jnp.logical_not(mine))
        def _():
            right_ref[n] = rights[1][pl.ds(row, states, stride=owned), :]


def join_tiles(wanted_ref, own_left, partner_left, right_ref, *out_refs):
    states = right_ref.shape[1]
    half = own_left.shape[0]
    owned = 2 * half
    base = lax.axis_index("dom") * owned
    lane = lax.broadcasted_iota(jnp.int32, (HALF, 2 * HALF), 1)
    is_left = lane < HALF
    gap = jnp.zeros((states, 2 * HALF - states), F32)
    below = jnp.zeros((HALF - states - 1, 2 * HALF), F32)
    place = 0
    for out_ref in out_refs:
        tall = HALF if len(out_ref.shape) == 3 else states + 1
        for n in range(out_ref.size // (tall * 2 * HALF)):
            part = wanted_ref[place]
            row = lax.rem(part, owned)
            mine = part - row == base

            def chosen(flag):
                return jnp.full((1, 2 * HALF), flag.astype(jnp.int32)) == 1

            second = row >= half
            at = jnp.where(second, row - half, row)
            left = jnp.where(chosen(mine), own_left[at], partner_left[at])
            left = jnp.where(chosen(second), pltpu.roll(left, HALF, 1), left)
            right = right_ref[place]
            right = jnp.concatenate(
                [jnp.concatenate([right, gap], axis=1), left[states + 1 : states + 2], below],
                axis=0,
            )
            tile = jnp.where(is_left, left, pltpu.roll(right, HALF, 1))
            if len(out_ref.shape) == 3:
                out_ref[n] = tile
            else:
                out_ref[pl.ds(n * (states + 1), states + 1), :] = tile[: states + 1]
            place += 1


def pick_tiles(wanted, tables, pieces):
    vmem = pl.BlockSpec(memory_space=pltpu.VMEM)
    count = wanted.shape[0] // pieces
    rows = tables[1].shape[0] + 1
    smem = pl.BlockSpec(memory_space=pltpu.SMEM)
    right = pl.pallas_call(
        copy_rights,
        in_specs=[smem, vmem, vmem],
        out_specs=vmem,
        out_shape=jax.ShapeDtypeStruct(wanted.shape + tables[1].shape[::2], F32),
        name="rights",
        compiler_params=LIMITS,
    )(wanted, tables[1], tables[3])
    return pl.pallas_call(
        join_tiles,
        in_specs=[smem] + [vmem] * 3,
        out_specs=[vmem] * pieces,
        out_shape=[jax.ShapeDtypeStruct((count * rows, 2 * HALF), F32)] * pieces,
        name="pick",
        compiler_params=LIMITS,
    )(wanted, tables[0], tables[2], right)


def start_split(skip, top_hbm, bottom_hbm, top_ref, bottom_ref, sems):
    chunks = sems.shape[1]
    chunk = top_ref.shape[0] // chunks

    def copies(g):
        there = pl.ds(g * chunk, chunk)
        here = pl.ds((skip + g) * chunk, chunk)
        return [
            pltpu.make_async_copy(src.at[here], dst.at[there], sems.at[i, g])
            for i, (src, dst) in enumerate(((top_hbm, top_ref), (bottom_hbm, bottom_ref)))
        ]

    for g in range(chunks):
        for copy in copies(g):
            copy.start()
    return copies


def finish_split(copies, out_ref, top_ref, bottom_ref, sems):
    nblocks = out_ref.shape[0]
    chunks = sems.shape[1]
    chunk = top_ref.shape[0] // chunks
    columns = out_ref.shape[3] // chunks
    fused = columns // BLK
    states = chunk // (fused * nblocks)
    pad = jnp.zeros((HALF - states, BLK), F32)

    def step(g, carry):
        for copy in copies(g):
            copy.wait()
        for b in range(fused):
            for n in range(nblocks):
                for side, ref in enumerate((top_ref, bottom_ref)):
                    first = g * chunk + b * states * nblocks + n
                    rows = ref[pl.ds(first, states, stride=nblocks), :]
                    full = jnp.concatenate([rows, pad], axis=0)
                    high = full.astype(BF16)
                    low = (full - high.astype(F32)).astype(BF16)
                    lanes = pl.ds(pl.multiple_of(g * columns + b * BLK, BLK), BLK)
                    out_ref[n, side, pl.ds(0, HALF), lanes] = high
                    out_ref[n, side, pl.ds(HALF, HALF), lanes] = low
        return carry

    lax.fori_loop(0, chunks, step, 0)


def early_kernel(top_hbm, bottom_hbm, out_ref, top_ref, bottom_ref, sems):
    copies = start_split(0, top_hbm, bottom_hbm, top_ref, bottom_ref, sems)
    finish_split(copies, out_ref, top_ref, bottom_ref, sems)


def late_kernel(
    skip,
    pair,
    rounds,
    blocks_hbm,
    chosen_hbm,
    lengths_hbm,
    padded_ref,
    top_hbm,
    bottom_hbm,
    own_left,
    own_right,
    partner_left,
    partner_right,
    out_ref,
    tiles_ref,
    aux_ref,
    map_ref,
    rows_ref,
    top_ref,
    bottom_ref,
    sems,
    right_ref,
    blocks_ref,
    chosen_ref,
    lengths_ref,
    small_sems,
):
    nblocks = out_ref.shape[0]
    branches = chosen_ref.shape[0]
    owned = own_right.shape[1]
    small = [
        pltpu.make_async_copy(src, dst, small_sems.at[i])
        for i, (src, dst) in enumerate(
            (
                (blocks_hbm, blocks_ref),
                (chosen_hbm, chosen_ref),
                (lengths_hbm, lengths_ref),
            )
        )
    ]
    for copy in small:
        copy.start()
    copies = start_split(skip, top_hbm, bottom_hbm, top_ref, bottom_ref, sems)
    for copy in small:
        copy.wait()
    copy_tiles(blocks_ref, own_left, own_right, partner_left, partner_right, tiles_ref, right_ref)
    my_pair = lax.axis_index("dom") // pair
    lane = lax.broadcasted_iota(jnp.int32, (1, BLK), 1)
    flat = lax.broadcasted_iota(jnp.int32, map_ref.shape, 0) * BLK
    flat = flat + lax.broadcasted_iota(jnp.int32, map_ref.shape, 1)
    for n in range(nblocks):
        part = blocks_ref[n]
        distance = lax.rem(lax.div(part, owned * pair) - my_pair + rounds, rounds)
        aux_ref[pl.ds(n, 1), :] = jnp.full((1, BLK), distance.astype(F32), F32)
        aux_ref[pl.ds(nblocks + n, 1), :] = jnp.full((1, BLK), part.astype(F32), F32)
    along = jnp.zeros((1, BLK), F32)
    update = jnp.zeros(map_ref.shape, jnp.int32)
    for b in range(branches):
        place = chosen_ref[b]
        time = lengths_ref[place]
        aux_ref[pl.ds(2 * nblocks + 8 + b, 1), :] = jnp.full((1, BLK), time, F32)
        along = jnp.where(lane == b, time, along)
        update = jnp.where(flat == place, b + 1, update)
    aux_ref[pl.ds(2 * nblocks, 1), :] = along
    map_ref[...] = update
    rows_ref[...] = padded_ref[...]
    finish_split(copies, out_ref, top_ref, bottom_ref, sems)


def split_scratch(top, branches, taken, fused):
    rows = top.shape[0] // branches * taken
    return [
        pltpu.VMEM((rows, BLK), F32),
        pltpu.VMEM((rows, BLK), F32),
        pltpu.SemaphoreType.DMA((2, taken // fused)),
    ]


def prepare_early(top, bottom, nblocks, branches, taken):
    hbm = pl.BlockSpec(memory_space=pltpu.HBM)
    return pl.pallas_call(
        early_kernel,
        in_specs=[hbm, hbm],
        out_specs=pl.BlockSpec(memory_space=pltpu.VMEM),
        out_shape=jax.ShapeDtypeStruct((nblocks, 2, 2 * HALF, taken * BLK), BF16),
        scratch_shapes=split_scratch(top, branches, taken, 2),
        name="early",
        compiler_params=LIMITS,
    )(in_hbm(top), in_hbm(bottom))


def prepare_late(
    blocks, chosen, lengths, padded, top, bottom, tables, skipped, pair, rounds
):
    nblocks = blocks.shape[0]
    branches = chosen.shape[0]
    taken = branches - skipped
    hbm = pl.BlockSpec(memory_space=pltpu.HBM)
    vmem = pl.BlockSpec(memory_space=pltpu.VMEM)
    return pl.pallas_call(
        functools.partial(late_kernel, skipped // 2, pair, rounds),
        in_specs=[hbm, hbm, hbm, vmem, hbm, hbm] + [vmem] * 4,
        out_specs=[vmem] * 5,
        out_shape=[
            jax.ShapeDtypeStruct((nblocks, 2, 2 * HALF, taken * BLK), BF16),
            jax.ShapeDtypeStruct((nblocks, HALF, 2 * HALF), F32),
            jax.ShapeDtypeStruct((2 * nblocks + 8 + branches, BLK), F32),
            jax.ShapeDtypeStruct(padded.shape, jnp.int32),
            jax.ShapeDtypeStruct(padded.shape, F32),
        ],
        scratch_shapes=split_scratch(top, branches, taken, 2)
        + [
            pltpu.VMEM((nblocks,) + tables[1].shape[::2], F32),
            pltpu.SMEM(blocks.shape, jnp.int32),
            pltpu.SMEM(chosen.shape, jnp.int32),
            pltpu.SMEM(lengths.shape, F32),
            pltpu.SemaphoreType.DMA((3,)),
        ],
        name="late",
        compiler_params=LIMITS,
    )(
        in_hbm(blocks),
        in_hbm(chosen),
        in_hbm(lengths),
        padded,
        in_hbm(top),
        in_hbm(bottom),
        *tables,
    )


def block_kernel(rounds, states, pieces, piece, aux_ref, weight_ref, early_ref, late_ref, own_ref, *refs):
    tiles = refs[: rounds - 1]
    earlier = refs[rounds - 1 : rounds - 1 + (piece if piece == pieces - 1 else 0)]
    like_ref, terms_ref, partial_ref = refs[-3:]
    branches, count, _ = like_ref.shape
    nblocks = early_ref.shape[0]
    split = early_ref.shape[3]
    start = piece * count
    wide = 2 * BLK
    lane = lax.broadcasted_iota(jnp.int32, (HALF, 2 * HALF), 1)
    is_left = lane < HALF
    for m in range(count):
        n = start + m
        distance = aux_ref[pl.ds(n, 1), :]
        tile = own_ref[n]
        for r in range(1, rounds):
            sent = tiles[r - 1][pl.ds(m * (states + 1), states + 1), :]
            sent = jnp.concatenate([sent, jnp.zeros((HALF - states - 1, 2 * HALF), F32)], axis=0)
            tile = jnp.where(distance == float(r), sent, tile)
        turned = pltpu.roll(tile, HALF, 1)
        flipped = tile[:, :HALF].T
        scaled = flipped * turned[states : states + 1, :HALF]
        left = jnp.concatenate([scaled, scaled], axis=1)
        sides = []
        for double in (left, jnp.where(is_left, turned, tile)):
            high = double.astype(BF16)
            low = (double - high.astype(F32)).astype(BF16)
            sides.append(jnp.concatenate([high, low[:, :HALF]], axis=1))
        expo = jnp.broadcast_to(flipped[:, states : states + 1], (HALF, BLK))
        powers = expo * LOG2_E
        for c in range(branches * BLK // wide):
            prods = []
            for side, lhs in enumerate(sides):
                if c * wide < split:
                    part = early_ref[n, side, :, pl.ds(c * wide, wide)]
                else:
                    part = late_ref[n, side, :, pl.ds(c * wide - split, wide)]
                rhs = jnp.concatenate([part, part[:HALF]], axis=0)
                prods.append(jnp.dot(lhs, rhs, preferred_element_type=F32))
            joint = prods[0] * prods[1]
            for h in range(wide // BLK):
                b = c * (wide // BLK) + h
                time = aux_ref[pl.ds(2 * nblocks + 8 + b, 1), :]
                zeroth = joint[:, h * BLK : (h + 1) * BLK] * jnp.exp2(powers * time)
                first = zeroth * expo
                second = first * expo
                for i, term in enumerate((zeroth, first, second)):
                    total = term[:SUB]
                    for k in range(SUB, HALF, SUB):
                        total = total + term[k : k + SUB]
                    partial_ref[i, b, pl.ds(m * SUB, SUB), :] = total

    weight = weight_ref[pl.ds(start, count), :].astype(F32)
    lanes = lax.broadcasted_iota(jnp.int32, (count, BLK), 1)
    terms = jnp.where(lanes == 2 * branches, aux_ref[pl.ds(nblocks + start, count), :], 0.0)
    for b in range(branches):
        sums = []
        for i in range(3):
            total = partial_ref[i, b, pl.ds(0, count, stride=SUB), :]
            for j in range(1, SUB):
                total = total + partial_ref[i, b, pl.ds(j, count, stride=SUB), :]
            sums.append(total)
        like_ref[b] = sums[0]
        inverse = 1.0 / sums[0]
        first = sums[1] * inverse
        second = sums[2] * inverse - first * first
        one = jnp.sum(weight * first, axis=1, keepdims=True)
        two = jnp.sum(weight * second, axis=1, keepdims=True)
        terms = jnp.where(lanes == b, one, terms)
        terms = jnp.where(lanes == branches + b, two, terms)
    if piece < pieces - 1:
        terms_ref[...] = terms
    else:
        terms = [ref[...] for ref in earlier] + [terms]
        for d in range(terms_ref.shape[0]):
            for i in range(0, pieces, 2):
                pair = terms[i] + pltpu.roll(terms[i + 1], HALF, 1)
                terms_ref[d, pl.ds(i // 2 * count, count), :] = pair


def block_likelihoods(
    aux, weight, operands, own_tiles, tiles, earlier, branches, states, devices, pieces, piece
):
    nblocks = operands[0].shape[0]
    count = nblocks // pieces
    vmem = pl.BlockSpec(memory_space=pltpu.VMEM)
    last = piece == pieces - 1
    return pl.pallas_call(
        functools.partial(block_kernel, len(tiles) + 1, states, pieces, piece),
        in_specs=[vmem] * (5 + len(tiles) + len(earlier)),
        out_specs=[vmem] * 2,
        out_shape=[
            jax.ShapeDtypeStruct((branches, count, BLK), F32),
            jax.ShapeDtypeStruct((devices, nblocks // 2, BLK) if last else (count, BLK), F32),
        ],
        scratch_shapes=[pltpu.VMEM((3, branches, count * SUB, BLK), F32)],
        name="blocks",
        compiler_params=LIMITS,
    )(aux, weight, *operands, own_tiles, *tiles, *earlier)


def sum_kernel(aux_ref, map_ref, lengths_ref, weight_ref, share_ref, *refs):
    like_refs = refs[:-3]
    part_ref, new_ref, loglik_ref = refs[-3:]
    branches, count, _ = like_refs[0].shape
    nblocks = count * len(like_refs)
    owned = part_ref.shape[1]
    terms = part_ref.shape[0]
    share = share_ref[...]
    share = jnp.concatenate([share, pltpu.roll(share, HALF, 1)], axis=0)
    share = share[:, :HALF]
    parts = lax.broadcasted_iota(jnp.int32, (share.shape[0], owned), 1)
    parts = parts + lax.axis_index("dom") * owned
    ident = share[:, terms : terms + 1].astype(jnp.int32)
    onehot = (ident == parts).astype(F32)
    sums = lax.dot_general(
        share,
        onehot,
        (((0,), (0,)), ((), ())),
        precision=lax.Precision.HIGHEST,
        preferred_element_type=F32,
    )
    part_ref[...] = sums[:terms]
    total = jnp.sum(share, axis=0, keepdims=True)
    total = jnp.concatenate([total, total], axis=1)
    second = pltpu.roll(total, BLK - branches, 1)
    updated = aux_ref[pl.ds(2 * nblocks, 1), :] - total / second
    lane = lax.broadcasted_iota(jnp.int32, (1, BLK), 1)
    place = map_ref[...]
    new = lengths_ref[...]
    for b in range(branches):
        value = jnp.sum(jnp.where(lane == b, updated, 0.0), axis=1, keepdims=True)
        new = jnp.where(place == b + 1, value, new)
    new_ref[...] = new
    for i, like_ref in enumerate(like_refs):
        blocks = pl.ds(i * count, count)
        weight = weight_ref[blocks, :].astype(F32)
        for b in range(branches):
            loglik_ref[b, blocks, :] = weight * jnp.log(like_ref[b])


def add_up(aux, places, lengths, weight, share, likes, owned):
    vmem = pl.BlockSpec(memory_space=pltpu.VMEM)
    branches = likes[0].shape[0]
    nblocks = weight.shape[0]
    return pl.pallas_call(
        sum_kernel,
        in_specs=[vmem] * (5 + len(likes)),
        out_specs=[vmem] * 3,
        out_shape=[
            jax.ShapeDtypeStruct((2 * branches, owned), F32),
            jax.ShapeDtypeStruct(lengths.shape, F32),
            jax.ShapeDtypeStruct((branches, nblocks, BLK), F32),
        ],
        name="sums",
        compiler_params=LIMITS,
    )(aux, places, lengths, weight, share, *likes)


def compute(
    top_partial,
    bottom_partial,
    left_vectors,
    right_vectors,
    decay_rates,
    state_weights,
    part_rates,
    branch_lengths,
    pattern_weights,
    block_partition,
    chosen_branches,
):
    branches, states, _, sites_here = top_partial.shape
    nblocks = sites_here // BLK
    owned = left_vectors.shape[0]
    groups = lax.axis_size("dom")
    pair = 2 if groups % 2 == 0 else 1
    rounds = groups // pair

    def shifted(value, r):
        step = [
            (d, ((d // pair + r) % rounds) * pair + d % pair) for d in range(groups)
        ]
        return lax.ppermute(value, "dom", step)

    blocks = block_partition[0]
    requests = [shifted(blocks, rounds - r) for r in range(1, rounds)]
    left_turned = jnp.transpose(left_vectors, (1, 0, 2))
    right_turned = jnp.transpose(right_vectors, (1, 0, 2))

    def swapped(value):
        if pair == 1:
            return value
        return lax.ppermute(value, "dom", [(d, d ^ 1) for d in range(groups)])

    partner_right = swapped(right_turned)
    own = pack_tables(left_turned, right_turned, decay_rates, state_weights, part_rates)
    partner_left = swapped(own[0])
    tables = [*own, partner_left, partner_right]
    pieces = 2
    answers = []
    for r, request in zip(range(1, rounds), requests):
        answers.append([shifted(t, r) for t in pick_tiles(request, tables, pieces)])
    count = branch_lengths.shape[0]
    rows = -(-count // BLK)
    padded = jnp.pad(branch_lengths, (0, rows * BLK - count)).reshape(rows, BLK)
    top = top_partial.reshape(branches * states * nblocks, BLK)
    bottom = bottom_partial.reshape(branches * states * nblocks, BLK)
    early = prepare_early(top, bottom, nblocks, branches, EARLY)
    late, tiles, aux, places, lengths = prepare_late(
        blocks,
        chosen_branches,
        branch_lengths,
        padded,
        top,
        bottom,
        tables,
        EARLY,
        pair,
        rounds,
    )
    operands = [early, late]
    answers = answers[::-1]
    devices = lax.axis_size("site") * groups
    weight = pattern_weights.reshape(nblocks, BLK)
    likes, earlier = [], []
    for piece in range(pieces):
        like, terms = block_likelihoods(
            aux,
            weight,
            operands,
            tiles,
            [answer[piece] for answer in answers],
            earlier,
            branches,
            states,
            devices,
            pieces,
            piece,
        )
        likes.append(like)
        earlier.append(terms)
    everything = lax.all_to_all(
        terms, ("site", "dom"), split_axis=0, concat_axis=0, tiled=True
    )
    parts, new_lengths, loglik = add_up(
        aux, places, lengths, weight, everything.reshape(-1, BLK), likes, owned
    )
    new_lengths = new_lengths.reshape(rows * BLK)[:count]
    return (
        loglik.reshape(branches, 1, sites_here),
        parts.reshape(2, branches, owned),
        new_lengths,
    )


def solution(mesh):
    return jax.shard_map(
        compute,
        mesh=mesh,
        in_specs=(
            P(None, None, "dom", "site"),
            P(None, None, "dom", "site"),
            P("dom", None, None),
            P("dom", None, None),
            P("dom", None),
            P("dom", None),
            P("dom"),
            P(),
            P("dom", "site"),
            P("dom", "site"),
            P(),
        ),
        out_specs=(P(None, "dom", "site"), P(None, None, "dom"), P()),
        check_vma=False,
    )
```
